32 devices in a mesh: samp: 16 (over z, x, core), var: 2 (over y).
Axes of the slice: x: 2, y: 2, z: 4, core: 2. Of those that a mesh axis runs over, the one named last changes fastest.
Arguments:
- genotypes: bfloat16 [17280, 8192], P('samp', 'var'), may hold values from 0 to 2, as said below
- residual: float32 [17280, 256], P('samp'), may hold values from -6 to 6
- coefficients: float32 [256, 8192], P('samp', 'var'), may hold values from -0.06 to 0.06
- penalty: float32 [8192], P('var'), may hold values from 0.2 to 3
- colors: int32 [2, 2], P(None, 'var'), may hold values from 0 to 1
Outputs:
- coefficients_out: float32 [256, 8192], P('samp', 'var')
- residual_out: float32 [17280, 256], P('samp')
The draws below stay inside these ranges and needn't reach their ends.
Inputs may be any that keep to these rules, and one draw needn't show every extreme that they name: `genotypes`: dosages of a genotype, whole numbers. `colors`: entry (r, v) names which of the 2 blocks of group v is updated in round r.
All inputs are finite; a program needn't handle non-finite values.
Results may differ from the reference program's by a relative error of at most 0.014.
Values may be sent and summed in bfloat16 or wider, within the bound.
No kernel may reach another device: no remote copies, remote signals or barrier semaphores. Data moves between devices by JAX's collectives and lax.ppermute only.
A program may use at most 64 MiB of HBM per device.

```python
import math
import jax
import jax.numpy as jnp
from jax import lax

K = 256
BS = 2048
NBLK_DEV = 2
ROUNDS = 2
SAMP_DEV = 1080
SAMPLES = 17280
VARIANTS = 8192
N_VAR = 2


def draw_genotypes(key, part):
    freq_key = jax.random.fold_in(key, 11)
    allele_key = jax.random.fold_in(key, 12)
    groups = SAMPLES // SAMP_DEV
    frequency = jax.random.randint(freq_key, (groups, VARIANTS), 5, 51)

    def one_group(group_index):
        draws = jax.random.randint(jax.random.fold_in(allele_key, group_index), (SAMP_DEV, VARIANTS), 0, 10000)
        limit = frequency[group_index][None, :]
        first_allele = (draws % 100 < limit).astype(jnp.int32)
        second_allele = (draws // 100 < limit).astype(jnp.int32)
        return (first_allele + second_allele).astype(jnp.float32).astype(jnp.bfloat16)
    stacked = lax.map(one_group, jnp.arange(groups, dtype=jnp.int32))
    return stacked.reshape(SAMPLES, VARIANTS)


def place_ends(result, own_key, low, largest):
    longest = result.shape.index(max(result.shape))
    spots = []
    for shift in (0, 1):
        where = [jax.random.randint(jax.random.fold_in(own_key, axis), (), 0, length) for axis, length in enumerate(result.shape)]
        where[longest] = (where[longest] + shift) % result.shape[longest]
        spots.append(tuple(where))
    return result.at[spots[0]].set(low).at[spots[1]].set(largest)


def block_scale(rng, dims, pieces, smallest, largest):
    def one(position, shards_of):
        steps = jax.random.uniform(jax.random.fold_in(jax.random.fold_in(rng, 6), position), (shards_of,), jnp.float32, smallest / len(pieces), largest / len(pieces))
        return jnp.repeat(jnp.exp(steps), dims[position] // shards_of).reshape((-1,) + (1,) * (len(dims) - position - 1))

    factor_of = one(*pieces[0])
    for cut in pieces[1:]:
        factor_of = factor_of * one(*cut)
    return factor_of


def bell_draw(stream_key, dims, width, most, cuts=(), held_as=jnp.bfloat16):
    gain = block_scale(stream_key, dims, cuts, -0.22, 0.18) if cuts else 1.0
    array = jax.random.normal(stream_key, dims, jnp.float32) * width * gain
    return jnp.minimum(jnp.maximum(array, -most), most).astype(held_as)


def setup_inputs(seed: int = 0) -> dict:
    splits = jax.random.split(jax.random.key(seed), 6)
    genotypes = draw_genotypes(jax.random.fold_in(splits[5], 71), 0)
    residual = bell_draw(splits[1], (SAMPLES, K), 1.0, 6.0, ((0, 16),), jnp.float32)
    coefficients = bell_draw(splits[2], (K, VARIANTS), 0.01, 0.06, ((0, 16), (1, 2)), jnp.float32)
    penalty = jnp.clip(jnp.exp(math.log(3.0) - 2.7080502 * jax.random.uniform(splits[3], (VARIANTS,), jnp.float32) ** block_scale(splits[3], (VARIANTS,), ((0, 2),), -0.2, 0.2)), 0.2, 3.0)
    colors = place_ends(jax.random.randint(splits[4], (ROUNDS, N_VAR), 0, NBLK_DEV), jax.random.fold_in(splits[4], 1), 0, NBLK_DEV - 1).astype(jnp.int32)
    return dict(genotypes=genotypes, residual=residual, coefficients=coefficients, penalty=penalty, colors=colors)


def column_moments(block_values):
    wide = block_values.astype(jnp.float32)
    counts = lax.optimization_barrier(jnp.sum(wide, axis=0))
    squares = lax.optimization_barrier(jnp.sum(wide * wide, axis=0))
    return (counts, squares)

def reference(genotypes, residual, coefficients, penalty, colors):
    group_width = NBLK_DEV * BS
    for round_index in range(ROUNDS):
        rounded = residual.astype(jnp.bfloat16)
        correction = jnp.zeros(residual.shape, jnp.float32)
        for group_index in range(N_VAR):
            first_column = (group_index * group_width + colors[round_index, group_index] * BS).astype(jnp.int32)
            block_values = lax.dynamic_slice_in_dim(genotypes, first_column, BS, 1)
            counts, squares = column_moments(block_values)
            column_mean = counts / SAMPLES
            column_scale = squares - counts * column_mean
            centered = (block_values.astype(jnp.float32) - column_mean[None, :]).astype(jnp.bfloat16)
            gradient = lax.dot_general(rounded, centered, (((0,), (0,)), ((), ())), preferred_element_type=jnp.float32)
            old_rows = lax.dynamic_slice_in_dim(coefficients, first_column, BS, 1)
            shifted = old_rows + gradient / column_scale[None, :]
            group_norm = jnp.sqrt(lax.optimization_barrier(jnp.sum(shifted * shifted, axis=0)) + 1e-06)
            penalty_part = lax.dynamic_slice_in_dim(penalty, first_column, BS, 0)
            shrink = jnp.maximum(0.0, 1.0 - penalty_part * jnp.sqrt(K / column_scale) / group_norm)
            new_rows = shrink[None, :] * shifted
            coefficients = lax.dynamic_update_slice(coefficients, new_rows, (jnp.int32(0), first_column))
            change_rows = (new_rows - old_rows).astype(jnp.bfloat16)
            correction = correction + lax.dot_general(centered, change_rows, (((1,), (1,)), ((), ())), preferred_element_type=jnp.float32)
        residual = residual - correction
    return (coefficients, residual)
```

```python
import jax
import jax.numpy as jnp
from jax import lax
from jax.sharding import PartitionSpec as P

BS = 2048
ROUNDS = 2
F32 = jnp.float32
BF16 = jnp.bfloat16


def stage_radices(size):
    radices = []
    while len(radices) < 2 and size % 2 == 0:
        radices.append(2)
        size //= 2
    if size > 1:
        radices.append(size)
    return radices


class Stage:
    def __init__(self, size, radix, stride):
        self.size, self.radix, self.stride = size, radix, stride
        self.digit = (lax.axis_index("samp") // stride) % radix

    def partner(self, digit, step):
        if self.radix & (self.radix - 1) == 0:
            return digit ^ step
        return (digit + step) % self.radix

    def source(self, digit, step):
        if self.radix & (self.radix - 1) == 0:
            return digit ^ step
        return (digit - step) % self.radix

    def pairs(self, step):
        out = []
        for i in range(self.size):
            d = (i // self.stride) % self.radix
            out.append((i, i + (self.partner(d, step) - d) * self.stride))
        return out

    def send(self, value, step):
        return lax.ppermute(value, "samp", self.pairs(step))


def stages(size):
    out, stride = [], 1
    for radix in stage_radices(size):
        out.append(Stage(size, radix, stride))
        stride *= radix
    return out


def pick(parts, index):
    value = parts[0]
    for i in range(1, len(parts)):
        value = jnp.where(index == i, parts[i], value)
    return value


def split_cols(value, radix):
    width = value.shape[-1] // radix
    return [value[..., i * width : (i + 1) * width] for i in range(radix)]


def split_rows(value, radix):
    height = value.shape[-2] // radix
    return [value[..., i * height : (i + 1) * height, :] for i in range(radix)]


def ordered(stage, own, received):
    by_step = [own] + received
    out = []
    for digit in range(stage.radix):
        value = by_step[0]
        for step in range(1, stage.radix):
            value = jnp.where(stage.source(stage.digit, step) == digit, by_step[step], value)
        out.append(value)
    return out


def scatter_columns(value, all_stages):
    for stage in all_stages:
        parts = split_cols(value, stage.radix)
        own = pick(parts, stage.digit)
        received = [
            stage.send(pick(parts, stage.partner(stage.digit, step)), step)
            for step in range(1, stage.radix)
        ]
        value = jnp.concatenate(ordered(stage, own, received), axis=-2)
    return value


def return_rows(value, all_stages):
    for stage in reversed(all_stages):
        parts = split_rows(value, stage.radix)
        own = pick(parts, stage.digit)
        received = [
            stage.send(pick(parts, stage.partner(stage.digit, step)), step)
            for step in range(1, stage.radix)
        ]
        value = jnp.concatenate(ordered(stage, own, received), axis=-1)
    return value


def gather_columns(value, all_stages):
    for stage in reversed(all_stages):
        received = [stage.send(value, step) for step in range(1, stage.radix)]
        value = jnp.concatenate(ordered(stage, value, received), axis=-1)
    return value


def rounded_to_bf16(value):
    return lax.reduce_precision(value, 8, 7)


def split_bf16(value, terms):
    out = []
    for _ in range(terms):
        top = rounded_to_bf16(value)
        out.append(top.astype(BF16))
        value = value - top
    return out


def reduce_scatter_gradient(partial, resid_sum, counts, twos, samples, all_stages):
    phenotypes = partial.shape[0]
    for stage in all_stages:
        width = partial.shape[1] // stage.radix
        cols = (split_cols(partial, stage.radix), split_cols(counts, stage.radix), split_cols(twos, stage.radix))
        sum_rows = [
            jnp.pad(row.reshape(-1, min(width, phenotypes)), ((0, 0), (0, max(0, width - phenotypes))))
            for row in split_bf16(resid_sum, 3)
        ]
        n_sum = sum_rows[0].shape[0]
        got = [(pick(cols[0], stage.digit), resid_sum, pick(cols[1], stage.digit), pick(cols[2], stage.digit))]
        for step in range(1, stage.radix):
            to = stage.partner(stage.digit, step)
            stats = split_bf16(pick(cols[1], to), 2) + split_bf16(pick(cols[2], to), 2)
            rows = [row[None, :] for row in stats] + sum_rows
            extra = jnp.concatenate(rows, axis=0)
            extra = jnp.pad(extra, ((0, -extra.shape[0] % 16), (0, 0)))
            message = jnp.concatenate([pick(cols[0], to).astype(BF16), extra], axis=0)
            message = stage.send(message, step)
            tail = message[phenotypes:].astype(F32)
            sums = tail[4 : 4 + 3 * n_sum].reshape(3, n_sum, -1)[:, :, : min(width, phenotypes)]
            got.append(
                (
                    message[:phenotypes].astype(F32),
                    jnp.sum(sums, axis=0).reshape(phenotypes),
                    tail[0] + tail[1],
                    tail[2] + tail[3],
                )
            )
        count_mean = sum(g[2] for g in got) / stage.radix
        sum_mean = sum(g[1] for g in got) / stage.radix
        total = sum(g[0] for g in got)
        for g in got:
            total = total + (g[1] - sum_mean)[:, None] * ((g[2] - count_mean) / samples)[None, :]
        partial = total
        resid_sum = sum(g[1] for g in got)
        counts = sum(g[2] for g in got)
        twos = sum(g[3] for g in got)
        samples = samples * stage.radix
    return partial, counts, twos, samples


def sum_over_var(value):
    size = lax.axis_size("var")
    if size & (size - 1):
        return lax.psum(value, "var")
    step = 1
    while step < size:
        sent = value.astype(BF16)
        other = lax.ppermute(sent, "var", [(i, i ^ step) for i in range(size)])
        value = rounded_to_bf16(value) + other.astype(F32)
        step *= 2
    return value


def shards(genotypes, residual, coefficients, penalty, colors):
    samp = lax.axis_size("samp")
    local_samples = genotypes.shape[0]
    rows_own = coefficients.shape[0]
    phenotypes = rows_own * samp
    blocks = genotypes.shape[1] // BS
    width = BS // samp
    all_stages = stages(samp)

    old_blocks = jnp.stack(
        [lax.dynamic_slice_in_dim(coefficients, colors[r, 0] * BS, BS, 1) for r in range(ROUNDS)]
    )
    old_columns = scatter_columns(old_blocks, all_stages)

    first = jnp.int32(0)
    for stage in all_stages:
        first = first * stage.radix + stage.digit
    first = first * width

    new_columns = []
    for r in range(ROUNDS):
        start = colors[r, 0] * BS
        values = lax.dynamic_slice_in_dim(genotypes, start, BS, 1)
        wide = values.astype(F32)
        counts = jnp.sum(wide, axis=0)
        squares = jnp.sum(wide * wide, axis=0)
        twos = 0.5 * (squares - counts)
        rounded = residual.astype(BF16)
        resid_sum = jnp.sum(rounded.astype(F32), axis=0)
        product = lax.dot_general(rounded, values, (((0,), (0,)), ((), ())), preferred_element_type=F32)
        partial = product - resid_sum[:, None] * (counts / local_samples)[None, :]
        gradient, counts, twos, total = reduce_scatter_gradient(
            partial, resid_sum, counts, twos, local_samples, all_stages
        )
        mean = counts / total
        scale = (counts + 2.0 * twos) - counts * mean
        old = old_columns[r]
        for before in range(r):
            old = jnp.where(colors[before, 0] == colors[r, 0], new_columns[before], old)
        weight = lax.dynamic_slice_in_dim(penalty, start + first, width, 0)
        shifted = old + gradient / scale[None, :]
        norm = jnp.sqrt(jnp.sum(shifted * shifted, axis=0) + 1e-06)
        shrink = jnp.maximum(0.0, 1.0 - weight * jnp.sqrt(phenotypes / scale) / norm)
        new = shrink[None, :] * shifted
        new_columns.append(new)
        change = (new - old).astype(BF16)
        means = jnp.concatenate([row[None, :] for row in split_bf16(mean, 3)], axis=0)
        means = jnp.pad(means, ((0, 13), (0, 0)))
        gathered = gather_columns(jnp.concatenate([change, means], axis=0), all_stages)
        change, means = gathered[:phenotypes], gathered[phenotypes:]
        shift = jnp.sum(
            lax.dot_general(means, change, (((1,), (1,)), ((), ())), preferred_element_type=F32), axis=0
        )
        product = lax.dot_general(values, change, (((1,), (1,)), ((), ())), preferred_element_type=F32)
        residual = residual - sum_over_var(product - shift[None, :])

    new_rows = return_rows(jnp.stack(new_columns), all_stages)
    pieces = []
    for block in range(blocks):
        piece = coefficients[:, block * BS : (block + 1) * BS]
        for r in range(ROUNDS):
            piece = jnp.where(colors[r, 0] == block, new_rows[r], piece)
        pieces.append(piece)
    return (jnp.concatenate(pieces, axis=1), residual)


def solution(mesh):
    placed = (P("samp", "var"), P("samp", None), P("samp", "var"), P("var"), P(None, "var"))
    return jax.shard_map(
        shards,
        mesh=mesh,
        in_specs=placed,
        out_specs=(P("samp", "var"), P("samp", None)),
        check_vma=False,
    )
```

```python
import jax
import jax.numpy as jnp
from jax import lax
from jax.sharding import PartitionSpec as P

BS = 2048
ROUNDS = 2
F32 = jnp.float32
BF16 = jnp.bfloat16


def stage_radices(size):
    radices = []
    while len(radices) < 2 and size % 2 == 0:
        radices.append(2)
        size //= 2
    if size > 1:
        radices.append(size)
    return radices


class Stage:
    def __init__(self, size, radix, stride):
        self.size, self.radix, self.stride = size, radix, stride
        self.digit = (lax.axis_index("samp") // stride) % radix

    def partner(self, digit, step):
        if self.radix & (self.radix - 1) == 0:
            return digit ^ step
        return (digit + step) % self.radix

    def source(self, digit, step):
        if self.radix & (self.radix - 1) == 0:
            return digit ^ step
        return (digit - step) % self.radix

    def pairs(self, step):
        out = []
        for i in range(self.size):
            d = (i // self.stride) % self.radix
            out.append((i, i + (self.partner(d, step) - d) * self.stride))
        return out

    def send(self, value, step):
        return lax.ppermute(value, "samp", self.pairs(step))


def stages(size):
    out, stride = [], 1
    for radix in stage_radices(size):
        out.append(Stage(size, radix, stride))
        stride *= radix
    return out


def pick(parts, index):
    value = parts[0]
    for i in range(1, len(parts)):
        value = jnp.where(index == i, parts[i], value)
    return value


def split_cols(value, radix):
    width = value.shape[-1] // radix
    return [value[..., i * width : (i + 1) * width] for i in range(radix)]


def ordered(stage, own, received):
    by_step = [own] + received
    out = []
    for digit in range(stage.radix):
        value = by_step[0]
        for step in range(1, stage.radix):
            value = jnp.where(stage.source(stage.digit, step) == digit, by_step[step], value)
        out.append(value)
    return out


def rounded_to_bf16(value):
    return lax.reduce_precision(value, 8, 7)


def split_bf16(value, terms):
    out = []
    for _ in range(terms):
        top = rounded_to_bf16(value)
        out.append(top.astype(BF16))
        value = value - top
    return out


def after(value, *others):
    return lax.optimization_barrier((value, *others))[0]


def scatter_stage(value, stage):
    parts = split_cols(value, stage.radix)
    own = pick(parts, stage.digit)
    received = [
        stage.send(pick(parts, stage.partner(stage.digit, step)), step) for step in range(1, stage.radix)
    ]
    return jnp.concatenate(ordered(stage, own, received), axis=-2)


def return_stage(value, stage, rows_axis):
    parts = [
        lax.index_in_dim(value, i, rows_axis, keepdims=True) for i in range(stage.radix)
    ]
    own = pick(parts, stage.digit)
    received = [
        stage.send(pick(parts, stage.partner(stage.digit, step)), step) for step in range(1, stage.radix)
    ]
    return ordered(stage, own, received)


def gather_stage(value, stage):
    received = [stage.send(value, step) for step in range(1, stage.radix)]
    return jnp.concatenate(ordered(stage, value, received), axis=-1)


def pad_rows(rows):
    return jnp.pad(rows, ((0, -rows.shape[0] % 16), (0, 0)))


class Moments:
    def __init__(self, counts, twos, samples):
        self.counts, self.twos, self.samples = counts, twos, samples


def sum_rows(resid_sum, width):
    size = resid_sum.shape[0]
    fit = min(width, size)
    rows = [
        jnp.pad(row.reshape(-1, fit), ((0, 0), (0, width - fit))) for row in split_bf16(resid_sum, 3)
    ]
    return jnp.concatenate(rows, axis=0)


def read_sums(rows, width, size):
    fit = min(width, size)
    return jnp.sum(rows.astype(F32).reshape(3, size // fit, width)[:, :, :fit], axis=0).reshape(size)


def merge_stage(stage, partial, resid_sum, counts, twos, samples, known=None):
    size, width = partial.shape[0], partial.shape[1] // stage.radix
    parts = split_cols(partial, stage.radix)
    count_parts, two_parts = split_cols(counts, stage.radix), split_cols(twos, stage.radix)
    sums = sum_rows(resid_sum, width)
    n_sum = sums.shape[0]
    partials = [pick(parts, stage.digit)]
    resid_sums = [resid_sum]
    moments = [(pick(count_parts, stage.digit), pick(two_parts, stage.digit))] if known is None else known
    sent = []
    for step in range(1, stage.radix):
        to = stage.partner(stage.digit, step)
        extra = sums
        if known is None:
            stats = split_bf16(pick(count_parts, to), 2) + split_bf16(pick(two_parts, to), 2)
            extra = jnp.concatenate([sums] + [row[None, :] for row in stats], axis=0)
        message = jnp.concatenate([pick(parts, to).astype(BF16), pad_rows(extra)], axis=0)
        sent.append(message)
        message = stage.send(message, step)
        partials.append(message[:size].astype(F32))
        tail = message[size:]
        resid_sums.append(read_sums(tail[:n_sum], width, size))
        if known is None:
            stats = tail[n_sum : n_sum + 4].astype(F32)
            moments.append((stats[0] + stats[1], stats[2] + stats[3]))
    count_mean = sum(m[0] for m in moments) / stage.radix
    sum_mean = sum(resid_sums) / stage.radix
    total = sum(partials)
    for s, m in zip(resid_sums, moments):
        total = total + (s - sum_mean)[:, None] * ((m[0] - count_mean) / samples)[None, :]
    return total, sum(resid_sums), moments, sent


def over_var(value):
    size = lax.axis_size("var")
    if size & (size - 1):
        total = lax.psum(value, "var")
        return total, jnp.zeros_like(total)
    step, other = 1, jnp.zeros_like(value)
    while step < size:
        value = value + other
        other = lax.ppermute(value.astype(BF16), "var", [(i, i ^ step) for i in range(size)]).astype(F32)
        value = rounded_to_bf16(value)
        step *= 2
    return value, other


def descent(genotypes, residual, coefficients, penalty, colors):
    samp = lax.axis_size("samp")
    local_samples = genotypes.shape[0]
    rows_own = coefficients.shape[0]
    phenotypes = rows_own * samp
    blocks = genotypes.shape[1] // BS
    width = BS // samp
    all_stages = stages(samp)
    early, last = all_stages[:-1], all_stages[-1]
    chunks = 2 if phenotypes % 256 == 0 else 1
    size = phenotypes // chunks

    old_columns = jnp.stack(
        [lax.dynamic_slice_in_dim(coefficients, colors[r, 0] * BS, BS, 1) for r in range(ROUNDS)]
    )
    for stage in early:
        old_gate = old_columns
        old_columns = scatter_stage(old_columns, stage)

    first = jnp.int32(0)
    for stage in all_stages:
        first = first * stage.radix + stage.digit
    first = first * width

    residuals = [residual[:, c * size : (c + 1) * size] for c in range(chunks)]
    pending = None
    new_columns = []
    gate = None
    for r in range(ROUNDS):
        start = colors[r, 0] * BS
        values = lax.dynamic_slice_in_dim(genotypes, start, BS, 1)
        seen = values if gate is None else lax.dynamic_slice_in_dim(after(genotypes, gate), start, BS, 1)
        wide = seen.astype(F32)
        counts = jnp.sum(wide, axis=0)
        twos = 0.5 * (jnp.sum(wide * wide, axis=0) - counts)
        local_mean = counts / local_samples

        partials, resid_sums, learned = [], [], []
        for c in range(chunks):
            if pending is not None:
                own, other = pending[c]
                if c:
                    other = after(other, *ahead)
                residuals[c] = residuals[c] - (own + other)
            rounded = residuals[c].astype(BF16)
            if r == 0:
                rounded = after(rounded, *([old_gate] if c == 0 else ahead))
            resid_sum = jnp.sum(rounded.astype(F32), axis=0)
            product = lax.dot_general(
                rounded, values, (((0,), (0,)), ((), ())), preferred_element_type=F32
            )
            partial = product - resid_sum[:, None] * local_mean[None, :]
            col_counts, col_twos, samples = counts, twos, local_samples
            for i, stage in enumerate(early):
                partial, resid_sum, moments, ahead = merge_stage(
                    stage,
                    partial,
                    resid_sum,
                    col_counts,
                    col_twos,
                    samples,
                    learned[i] if c else None,
                )
                if not c:
                    learned.append(moments)
                col_counts = sum(m[0] for m in learned[i])
                col_twos = sum(m[1] for m in learned[i])
                samples = samples * stage.radix
            partials.append(partial)
            resid_sums.append(resid_sum)
        if r == 0:
            old_columns = scatter_stage(old_columns, last)
        gradient, _, moments, _ = merge_stage(
            last,
            jnp.concatenate(partials, axis=0),
            jnp.concatenate(resid_sums, axis=0),
            col_counts,
            col_twos,
            samples,
        )
        counts = sum(m[0] for m in moments)
        twos = sum(m[1] for m in moments)
        total = local_samples * samp
        mean = counts / total
        scale = (counts + 2.0 * twos) - counts * mean
        old = old_columns[r]
        for before in range(r):
            old = jnp.where(colors[before, 0] == colors[r, 0], new_columns[before], old)
        weight = lax.dynamic_slice_in_dim(penalty, start + first, width, 0)
        shifted = old + gradient / scale[None, :]
        norm = jnp.sqrt(jnp.sum(shifted * shifted, axis=0) + 1e-06)
        shrink = jnp.maximum(0.0, 1.0 - weight * jnp.sqrt(phenotypes / scale) / norm)
        new = shrink[None, :] * shifted
        new_columns.append(new)
        change = (new - old).astype(BF16)
        means = pad_rows(jnp.concatenate([row[None, :] for row in split_bf16(mean, 3)], axis=0))
        message = jnp.concatenate([means, change], axis=0)
        gate = message
        gathered = gather_stage(message, last)
        lead = means.shape[0]
        cuts = [0] + [lead + size * (c + 1) for c in range(chunks)]
        pieces = [gathered[cuts[c] : cuts[c + 1]] for c in range(chunks)]
        received = []
        top = len(early) - 1
        for c in range(chunks):
            received.append([early[top].send(pieces[c], step) for step in range(1, early[top].radix)])
        pending = []
        for c in range(chunks):
            if c:
                received[c] = [after(value, product) for value in received[c]]
            piece = jnp.concatenate(ordered(early[top], pieces[c], received[c]), axis=-1)
            for i in reversed(range(top)):
                piece = gather_stage(piece, early[i])
            if c == 0:
                mean_rows, piece = piece[:lead], piece[lead:]
            shift = jnp.sum(
                lax.dot_general(
                    mean_rows, piece, (((1,), (1,)), ((), ())), preferred_element_type=F32
                ),
                axis=0,
            )
            product = lax.dot_general(
                values, piece, (((1,), (1,)), ((), ())), preferred_element_type=F32
            )
            product = product - shift[None, :]
            pending.append(over_var(product))

    for c in range(chunks):
        own, other = pending[c]
        residuals[c] = residuals[c] - (own + other)
    digits = [stage.radix for stage in reversed(all_stages)]
    home = after(jnp.stack(new_columns), product)
    home = home.reshape([ROUNDS] + digits + [rows_own, width])
    pieces = [home]
    for i, stage in reversed(list(enumerate(all_stages))):
        axis = 1 + len(all_stages) - 1 - i
        pieces = [return_stage(piece, stage, axis) for piece in pieces][0]
        pieces = [jnp.concatenate(pieces, axis=-1)]
    new_rows = pieces[0].reshape(ROUNDS, rows_own, BS)
    out = []
    for block in range(blocks):
        piece = coefficients[:, block * BS : (block + 1) * BS]
        for r in range(ROUNDS):
            piece = jnp.where(colors[r, 0] == block, new_rows[r], piece)
        out.append(piece)
    return (jnp.concatenate(out, axis=1), jnp.concatenate(residuals, axis=1))


def solution(mesh):
    placed = (P("samp", "var"), P("samp", None), P("samp", "var"), P("var"), P(None, "var"))
    return jax.shard_map(
        descent,
        mesh=mesh,
        in_specs=placed,
        out_specs=(P("samp", "var"), P("samp", None)),
        check_vma=False,
    )
```

```python
import jax
import jax.numpy as jnp
from jax import lax
from jax.experimental import pallas as pl
from jax.experimental.pallas import tpu as pltpu
from jax.sharding import PartitionSpec as P

BS = 2048
ROUNDS = 2
F32 = jnp.float32
BF16 = jnp.bfloat16


def stage_radices(size):
    radices = []
    while len(radices) < 2 and size % 2 == 0:
        radices.append(2)
        size //= 2
    if size > 1:
        radices.append(size)
    return radices


class Stage:
    def __init__(self, size, radix, stride):
        self.size, self.radix, self.stride = size, radix, stride
        self.digit = (lax.axis_index("samp") // stride) % radix

    def partner(self, digit, step):
        if self.radix & (self.radix - 1) == 0:
            return digit ^ step
        return (digit + step) % self.radix

    def source(self, digit, step):
        if self.radix & (self.radix - 1) == 0:
            return digit ^ step
        return (digit - step) % self.radix

    def pairs(self, step):
        out = []
        for i in range(self.size):
            d = (i // self.stride) % self.radix
            out.append((i, i + (self.partner(d, step) - d) * self.stride))
        return out

    def send(self, value, step):
        return lax.ppermute(value, "samp", self.pairs(step))


def stages(size):
    out, stride = [], 1
    for radix in stage_radices(size):
        out.append(Stage(size, radix, stride))
        stride *= radix
    return out


def pick(parts, index):
    value = parts[0]
    for i in range(1, len(parts)):
        value = jnp.where(index == i, parts[i], value)
    return value


def split_cols(value, radix):
    width = value.shape[-1] // radix
    return [value[..., i * width : (i + 1) * width] for i in range(radix)]


def ordered(stage, own, received):
    by_step = [own] + received
    out = []
    for digit in range(stage.radix):
        value = by_step[0]
        for step in range(1, stage.radix):
            value = jnp.where(stage.source(stage.digit, step) == digit, by_step[step], value)
        out.append(value)
    return out


def rounded_to_bf16(value):
    return lax.reduce_precision(value, 8, 7)


def split_bf16(value, terms):
    out = []
    for _ in range(terms):
        top = rounded_to_bf16(value)
        out.append(top.astype(BF16))
        value = value - top
    return out


def after(value, *others):
    return lax.optimization_barrier((value, *others))[0]


def scatter_stage(value, stage, gate=()):
    parts = split_cols(value, stage.radix)
    own = pick(parts, stage.digit)
    received = [
        stage.send(pick(parts, stage.partner(stage.digit, step)), step) for step in range(1, stage.radix)
    ]
    received = [after(value, *gate) for value in received]
    return jnp.concatenate(ordered(stage, own, received), axis=-2)


def home_stage(value, stage, axis, gate=()):
    parts = [lax.index_in_dim(value, i, axis, keepdims=False) for i in range(stage.radix)]
    own = pick(parts, stage.digit)
    received = [
        stage.send(pick(parts, stage.partner(stage.digit, step)), step) for step in range(1, stage.radix)
    ]
    received = [after(value, *gate) for value in received]
    return jnp.stack(ordered(stage, own, received))


def gather_stage(value, stage):
    received = [stage.send(value, step) for step in range(1, stage.radix)]
    return jnp.concatenate(ordered(stage, value, received), axis=-1)


def pad_rows(rows):
    return jnp.pad(rows, ((0, -rows.shape[0] % 16), (0, 0)))


def sum_rows(resid_sum, width):
    size = resid_sum.shape[0]
    fit = min(width, size)
    rows = [
        jnp.pad(row.reshape(-1, fit), ((0, 0), (0, width - fit))) for row in split_bf16(resid_sum, 3)
    ]
    return jnp.concatenate(rows, axis=0)


def read_sums(rows, width, size):
    fit = min(width, size)
    return jnp.sum(rows.astype(F32).reshape(3, size // fit, width)[:, :, :fit], axis=0).reshape(size)


def merge_stage(stage, partial, resid_sum, stats, samples, known=None, gate=()):
    size, width = partial.shape[0], partial.shape[1] // stage.radix
    n_stats = stats.shape[0]
    parts = split_cols(partial, stage.radix)
    stat_parts = split_cols(stats, stage.radix)
    sums = sum_rows(resid_sum, width)
    n_sum = sums.shape[0]
    partials = [pick(parts, stage.digit)]
    resid_sums = [resid_sum]
    members = [pick(stat_parts, stage.digit)] if known is None else known
    sent = []
    for step in range(1, stage.radix):
        to = stage.partner(stage.digit, step)
        extra = sums
        if known is None:
            extra = jnp.concatenate([sums] + split_bf16(pick(stat_parts, to), 2), axis=0)
        message = jnp.concatenate([pick(parts, to).astype(BF16), pad_rows(extra)], axis=0)
        sent.append(message)
        message = after(stage.send(message, step), *gate)
        partials.append(message[:size].astype(F32))
        tail = message[size:]
        resid_sums.append(read_sums(tail[:n_sum], width, size))
        if known is None:
            terms = tail[n_sum : n_sum + 2 * n_stats].astype(F32)
            members.append(terms[:n_stats] + terms[n_stats:])
    count_mean = sum(m[0] for m in members) / stage.radix
    sum_mean = sum(resid_sums) / stage.radix
    total = sum(partials)
    for s, m in zip(resid_sums, members):
        total = total + (s - sum_mean)[:, None] * ((m[0] - count_mean) / samples)[None, :]
    return total, sum(resid_sums), members, sent


def sum_stage(stage, partial):
    parts = split_cols(partial, stage.radix)
    total = pick(parts, stage.digit)
    sent = []
    for step in range(1, stage.radix):
        sent.append(pick(parts, stage.partner(stage.digit, step)).astype(BF16))
        total = total + stage.send(sent[-1], step).astype(F32)
    return total, sent


TILES = 4


def head_kernel(columns, genotypes, residual, partial, stats, resid_sum, blocks, sems):
    samples, phenotypes = residual.shape
    width = BS // TILES

    def copy(r, t):
        at = pl.multiple_of(columns[r] * BS + t * width, width)
        return pltpu.make_async_copy(
            genotypes.at[:, pl.ds(at, width)], blocks.at[r, :, pl.ds(t * width, width)], sems.at[r, t]
        )

    for r in range(ROUNDS):
        for t in range(TILES):
            copy(r, t).start()
    rounded = residual[...].astype(BF16)
    sums = jnp.sum(rounded.astype(F32), axis=0, keepdims=True)
    resid_sum[...] = sums
    column = jnp.broadcast_to(jnp.transpose(jnp.broadcast_to(sums, (8, phenotypes)))[:, :1], (phenotypes, width))
    for r in range(ROUNDS):
        for t in range(TILES):
            copy(r, t).wait()
            here = pl.ds(t * width, width)
            values = blocks[r, :, here]
            wide = values.astype(F32)
            counts = jnp.sum(wide, axis=0, keepdims=True)
            squares = jnp.sum(wide * wide, axis=0, keepdims=True)
            stats[2 * r : 2 * r + 1, here] = counts
            stats[2 * r + 1 : 2 * r + 2, here] = 0.5 * (squares - counts)
            if r == 0:
                product = lax.dot_general(
                    rounded, values, (((0,), (0,)), ((), ())), preferred_element_type=F32
                )
                partial[:, here] = product - column * (counts * (1.0 / samples))


def head(columns, genotypes, residual):
    samples, phenotypes = residual.shape
    whole = pl.BlockSpec(memory_space=pltpu.VMEM)
    return pl.pallas_call(
        head_kernel,
        out_shape=[
            jax.ShapeDtypeStruct((phenotypes, BS), F32),
            jax.ShapeDtypeStruct((2 * ROUNDS, BS), F32),
            jax.ShapeDtypeStruct((1, phenotypes), F32),
        ],
        in_specs=[pl.BlockSpec(memory_space=pltpu.SMEM), pl.BlockSpec(memory_space=pltpu.HBM), whole],
        out_specs=[whole] * 3,
        scratch_shapes=[pltpu.VMEM((ROUNDS, samples, BS), BF16), pltpu.SemaphoreType.DMA((ROUNDS, TILES))],
        cost_estimate=pl.CostEstimate(
            flops=4 * samples * phenotypes * BS, bytes_accessed=4 * samples * BS, transcendentals=0
        ),
        compiler_params=pltpu.CompilerParams(vmem_limit_bytes=50 * 1024 * 1024),
        name="head",
    )(columns, genotypes, residual)


def over_var(value):
    size = lax.axis_size("var")
    if size & (size - 1):
        total = lax.psum(value, "var")
        return total, jnp.zeros_like(total)
    step, other = 1, jnp.zeros_like(value)
    while step < size:
        value = value + other
        other = lax.ppermute(value.astype(BF16), "var", [(i, i ^ step) for i in range(size)]).astype(F32)
        value = rounded_to_bf16(value)
        step *= 2
    return value, other


def chosen_block(genotypes, block, gate):
    genotypes = after(genotypes, gate)
    return lax.optimization_barrier(lax.dynamic_slice_in_dim(genotypes, block * BS, BS, 1))


def descent(genotypes, residual, coefficients, penalty, colors):
    samp = lax.axis_size("samp")
    rows_own = coefficients.shape[0]
    phenotypes = rows_own * samp
    local_samples, total_samples = genotypes.shape[0], genotypes.shape[0] * samp
    width = BS // samp
    all_stages = stages(samp)
    early, last = all_stages[:-1], all_stages[-1]
    top = len(early) - 1
    chunks = 2 if phenotypes % 256 == 0 else 1
    size = phenotypes // chunks
    chosen = colors[:, 0]

    olds = [lax.dynamic_slice_in_dim(coefficients, chosen[r] * BS, BS, 1) for r in range(ROUNDS)]
    old_columns = jnp.stack(olds)
    partial, stats, resid_sum = head(chosen, genotypes, residual)
    values = []
    partial_chunks = [partial[c * size : (c + 1) * size] for c in range(chunks)]
    sum_chunks = [resid_sum[0, c * size : (c + 1) * size] for c in range(chunks)]

    first = jnp.int32(0)
    for stage in all_stages:
        first = first * stage.radix + stage.digit
    first = first * width

    for i in range(top):
        old_columns = scatter_stage(old_columns, early[i])
    learned, moments, samples = [], stats, local_samples
    ahead = ()
    for c in range(chunks):
        gate = ahead
        here, moments, samples = (partial_chunks[c], sum_chunks[c]), stats, local_samples
        for i, stage in enumerate(early):
            *here, members, ahead = merge_stage(
                stage, *here, moments, samples, learned[i] if c else None, () if i else gate
            )
            if not c:
                learned.append(members)
            moments, samples = sum(learned[i]), samples * stage.radix
        partial_chunks[c], sum_chunks[c] = here
    old_columns = scatter_stage(old_columns, early[top], ahead)
    old = scatter_stage(old_columns[0], last)
    gradient, _, members, _ = merge_stage(
        last, jnp.concatenate(partial_chunks, axis=0), jnp.concatenate(sum_chunks), moments, samples
    )
    moments = sum(members)

    residuals = [residual[:, c * size : (c + 1) * size] for c in range(chunks)]
    news = []
    for r in range(ROUNDS):
        counts, twos = moments[2 * r], moments[2 * r + 1]
        mean = counts / total_samples
        scale = (counts + 2.0 * twos) - counts * mean
        if r:
            ahead = ()
            for c in range(chunks):
                own, other = pending[c]
                if c:
                    other = after(other, *ahead)
                residuals[c] = residuals[c] - (own + other)
                rounded = residuals[c].astype(BF16)
                resid_sum = jnp.sum(rounded.astype(F32), axis=0)
                partial = lax.dot_general(rounded, values[r], (((0,), (0,)), ((), ())), preferred_element_type=F32)
                partial = partial - resid_sum[:, None] * means[r][None, :]
                for stage in early:
                    partial, ahead = sum_stage(stage, partial)
                partial_chunks[c] = partial
            old = scatter_stage(after(old_columns[r], *ahead), last)
            gradient, _ = sum_stage(last, jnp.concatenate(partial_chunks, axis=0))
            for before in range(r):
                old = jnp.where(chosen[before] == chosen[r], news[before], old)
        weight = lax.dynamic_slice_in_dim(penalty, chosen[r] * BS + first, width, 0)
        shifted = old + gradient / scale[None, :]
        norm = jnp.sqrt(jnp.sum(shifted * shifted, axis=0) + 1e-06)
        shrink = jnp.maximum(0.0, 1.0 - weight * jnp.sqrt(phenotypes / scale) / norm)
        new = shrink[None, :] * shifted
        news.append(new)
        change = (new - old).astype(BF16)
        means_sent = [mean] if r else [moments[2 * i] / total_samples for i in range(ROUNDS)]
        rows = [row[None, :] for sent in means_sent for row in split_bf16(sent, 3)]
        rows = pad_rows(jnp.concatenate(rows, axis=0))
        lead = rows.shape[0]
        message = jnp.concatenate([rows, change], axis=0)
        if r == 0:
            values.append(chosen_block(genotypes, chosen[0], message))
        gathered = gather_stage(message, last)
        cuts = [0] + [lead + size * (c + 1) for c in range(chunks)]
        pieces = [gathered[cuts[c] : cuts[c + 1]] for c in range(chunks)]
        received = []
        for c in range(chunks):
            received.append([early[top].send(pieces[c], step) for step in range(1, early[top].radix)])
        pending = []
        for c in range(chunks):
            if c:
                received[c] = [after(value, product) for value in received[c]]
            piece = jnp.concatenate(ordered(early[top], pieces[c], received[c]), axis=-1)
            for i in reversed(range(top)):
                piece = gather_stage(piece, early[i])
            if c == 0:
                rows, piece = piece[:lead], piece[lead:]
                if r == 0:
                    means = [jnp.sum(rows[3 * i : 3 * i + 3].astype(F32), axis=0) for i in range(ROUNDS)]
            shift = lax.dot_general(
                rows[:3], piece, (((1,), (1,)), ((), ())), preferred_element_type=F32
            )
            shift = jnp.sum(shift, axis=0)
            product = lax.dot_general(
                values[r], piece, (((1,), (1,)), ((), ())), preferred_element_type=F32
            )
            product = product - shift[None, :]
            pending.append(over_var(product))
        if r + 1 < ROUNDS:
            values.append(chosen_block(genotypes, chosen[r + 1], product))

    for c in range(chunks):
        own, other = pending[c]
        residuals[c] = residuals[c] - (own + other)

    home = jnp.stack(news).reshape(
        [ROUNDS] + [stage.radix for stage in reversed(all_stages)] + [rows_own, width]
    )
    axes = list(reversed(range(len(all_stages))))
    found = []
    for i in [top, top + 1] + list(reversed(range(top))):
        axis = len(found) + 1 + axes.index(i)
        home = home_stage(home, all_stages[i], axis, [product] if i == top else ())
        axes.remove(i)
        found.insert(0, i)
    home = jnp.transpose(home, [found.index(i) for i in range(len(found))] + [len(found) + j for j in range(3)])
    home = home.reshape(samp, ROUNDS, rows_own, width)
    new_rows = [jnp.concatenate([home[s, r] for s in range(samp)], axis=-1) for r in range(ROUNDS)]
    out = []
    for block in range(genotypes.shape[1] // BS):
        piece = coefficients[:, block * BS : (block + 1) * BS]
        for r in range(ROUNDS):
            piece = jnp.where(chosen[r] == block, new_rows[r], piece)
        out.append(piece)
    return (jnp.concatenate(out, axis=1), jnp.concatenate(residuals, axis=1))


def solution(mesh):
    placed = (P("samp", "var"), P("samp", None), P("samp", "var"), P("var"), P(None, "var"))
    return jax.shard_map(
        descent,
        mesh=mesh,
        in_specs=placed,
        out_specs=(P("samp", "var"), P("samp", None)),
        check_vma=False,
    )
```

```python
import jax
import jax.numpy as jnp
from jax import lax
from jax.experimental import pallas as pl
from jax.experimental.pallas import tpu as pltpu
from jax.sharding import PartitionSpec as P

BS = 2048
ROUNDS = 2
F32 = jnp.float32
BF16 = jnp.bfloat16


def stage_radices(size):
    radices = []
    while len(radices) < 2 and size % 2 == 0:
        radices.append(2)
        size //= 2
    if size > 1:
        radices.append(size)
    return radices


class Stage:
    def __init__(self, size, radix, stride):
        self.size, self.radix, self.stride = size, radix, stride
        self.digit = (lax.axis_index("samp") // stride) % radix

    def partner(self, digit, step):
        if self.radix & (self.radix - 1) == 0:
            return digit ^ step
        return (digit + step) % self.radix

    def source(self, digit, step):
        if self.radix & (self.radix - 1) == 0:
            return digit ^ step
        return (digit - step) % self.radix

    def pairs(self, step):
        out = []
        for i in range(self.size):
            d = (i // self.stride) % self.radix
            out.append((i, i + (self.partner(d, step) - d) * self.stride))
        return out

    def send(self, value, step):
        return lax.ppermute(value, "samp", self.pairs(step))


def stages(size):
    out, stride = [], 1
    for radix in stage_radices(size):
        out.append(Stage(size, radix, stride))
        stride *= radix
    return out


def pick(parts, index):
    value = parts[0]
    for i in range(1, len(parts)):
        value = jnp.where(index == i, parts[i], value)
    return value


def split_cols(value, radix):
    width = value.shape[-1] // radix
    return [value[..., i * width : (i + 1) * width] for i in range(radix)]


def ordered(stage, own, received):
    by_step = [own] + received
    out = []
    for digit in range(stage.radix):
        value = by_step[0]
        for step in range(1, stage.radix):
            value = jnp.where(stage.source(stage.digit, step) == digit, by_step[step], value)
        out.append(value)
    return out


def rounded_to_bf16(value):
    return lax.reduce_precision(value, 8, 7)


def split_bf16(value, terms):
    out = []
    for _ in range(terms):
        top = rounded_to_bf16(value)
        out.append(top.astype(BF16))
        value = value - top
    return out


def after(value, *others):
    return lax.optimization_barrier((value, *others))[0]


def send_parts(stage, parts):
    own = pick(parts, stage.digit)
    sent = [pick(parts, stage.partner(stage.digit, step)) for step in range(1, stage.radix)]
    return own, [stage.send(sent[step - 1], step) for step in range(1, stage.radix)]


def in_order(stage, own, received, gate=()):
    return ordered(stage, own, [after(value, *gate) for value in received])


def gather_stage(value, stage, gate=()):
    received = [after(stage.send(value, step), *gate) for step in range(1, stage.radix)]
    return jnp.concatenate(ordered(stage, value, received), axis=-1)


def pad_rows(rows):
    return jnp.pad(rows, ((0, -rows.shape[0] % 16), (0, 0)))


def sum_rows(resid_sum, width):
    size = resid_sum.shape[0]
    fit = min(width, size)
    rows = [
        jnp.pad(row.reshape(-1, fit), ((0, 0), (0, width - fit))) for row in split_bf16(resid_sum, 3)
    ]
    return jnp.concatenate(rows, axis=0)


def read_sums(rows, width, size):
    fit = min(width, size)
    return jnp.sum(rows.astype(F32).reshape(3, size // fit, width)[:, :, :fit], axis=0).reshape(size)


def merge_stage(stage, partial, resid_sum, riders, stats, samples):
    size, width = partial.shape[0], partial.shape[1] // stage.radix
    parts = split_cols(partial, stage.radix)
    sums = sum_rows(resid_sum, width)
    n_sum = sums.shape[0]
    stat_parts = None if stats is None else split_cols(stats, stage.radix)
    rider_parts = None if riders is None else split_cols(riders, stage.radix)
    sent, arrived = [], []
    for step in range(1, stage.radix):
        to = stage.partner(stage.digit, step)
        extra = sums
        if stats is not None:
            extra = jnp.concatenate([sums] + split_bf16(pick(stat_parts, to), 2), axis=0)
        message = [pick(parts, to).astype(BF16), pad_rows(extra)]
        n_extra = message[1].shape[0]
        if riders is not None:
            message.append(pick(rider_parts, to))
        sent.append(jnp.concatenate(message, axis=0))
        arrived.append(stage.send(sent[-1], step))

    def finish(gate=(), members=None):
        partials, resid_sums, ridden = [pick(parts, stage.digit)], [resid_sum], []
        if stats is not None:
            n_stats = stats.shape[0]
            members = [pick(stat_parts, stage.digit)]
        for message in arrived:
            message = after(message, *gate)
            partials.append(message[:size].astype(F32))
            tail = message[size:]
            ridden.append(tail[n_extra:])
            resid_sums.append(read_sums(tail[:n_sum], width, size))
            if stats is not None:
                terms = tail[n_sum : n_sum + 2 * n_stats].astype(F32)
                members.append(terms[:n_stats] + terms[n_stats:])
        count_mean = sum(m[0] for m in members) / stage.radix
        sum_mean = sum(resid_sums) / stage.radix
        total = sum(partials)
        for s, m in zip(resid_sums, members):
            total = total + (s - sum_mean)[:, None] * ((m[0] - count_mean) / samples)[None, :]
        merged = None
        if riders is not None:
            merged = jnp.concatenate(ordered(stage, pick(rider_parts, stage.digit), ridden), axis=0)
        return (total, sum(resid_sums), merged), members

    return sent, finish


def sum_stage(stage, partial):
    parts = split_cols(partial, stage.radix)
    own = pick(parts, stage.digit)
    sent = [
        pick(parts, stage.partner(stage.digit, step)).astype(BF16) for step in range(1, stage.radix)
    ]
    arrived = [stage.send(sent[step - 1], step) for step in range(1, stage.radix)]

    def finish(gate=()):
        return sum((after(value, *gate).astype(F32) for value in arrived), start=own)

    return sent, finish


TILES = 4
GROUP = 64


def column_moments(values):
    rows, width = values.shape
    whole = rows // 16 * 16
    counts = jnp.zeros((1, width), F32)
    twos = jnp.zeros((1, width), F32)
    one, zero = jnp.bfloat16(1), jnp.bfloat16(0)
    for begin in range(0, whole, 16 * GROUP):
        count_sum = two_sum = None
        for at in range(begin, min(begin + 16 * GROUP, whole), 16):
            part = values[at : at + 16]
            above = jnp.maximum(part - one, zero)
            count_sum = part if count_sum is None else count_sum + part
            two_sum = above if two_sum is None else two_sum + above
        counts = counts + jnp.sum(count_sum.astype(F32), axis=0, keepdims=True)
        twos = twos + jnp.sum(two_sum.astype(F32), axis=0, keepdims=True)
    if whole < rows:
        part = values[whole:].astype(F32)
        counts = counts + jnp.sum(part, axis=0, keepdims=True)
        twos = twos + jnp.sum(jnp.maximum(part - 1.0, 0.0), axis=0, keepdims=True)
    return counts, twos


def head_kernel(
    colors, genotypes, residual, coefficients, partial, stats, resid_sum, olds, blocks, resid, sems, resid_sem, old_sems
):
    samples, phenotypes = residual.shape
    width = BS // TILES

    def copy(r, t):
        at = pl.multiple_of(colors[r, 0] * BS + t * width, width)
        return pltpu.make_async_copy(
            genotypes.at[:, pl.ds(at, width)], blocks.at[r, :, pl.ds(t * width, width)], sems.at[r, t]
        )

    def old_copy(r):
        at = pl.multiple_of(colors[r, 0] * BS, BS)
        return pltpu.make_async_copy(coefficients.at[:, pl.ds(at, BS)], olds.at[r], old_sems.at[r])

    resid_copy = pltpu.make_async_copy(residual, resid, resid_sem)
    resid_copy.start()
    for r in range(ROUNDS):
        for t in range(TILES):
            copy(r, t).start()
        old_copy(r).start()
    resid_copy.wait()
    rounded = resid[...].astype(BF16)
    sums = jnp.sum(rounded.astype(F32), axis=0, keepdims=True)
    resid_sum[...] = sums
    column = jnp.broadcast_to(jnp.transpose(jnp.broadcast_to(sums, (8, phenotypes)))[:, :1], (phenotypes, width))
    for r in range(ROUNDS):
        for t in range(TILES):
            copy(r, t).wait()
            here = pl.ds(t * width, width)
            values = blocks[r, :, here]
            counts, twos = column_moments(values)
            stats[2 * r : 2 * r + 1, here] = counts
            stats[2 * r + 1 : 2 * r + 2, here] = twos
            if r == 0:
                product = lax.dot_general(
                    rounded, values, (((0,), (0,)), ((), ())), preferred_element_type=F32
                )
                partial[:, here] = product - column * (counts * (1.0 / samples))
        old_copy(r).wait()


def head(colors, genotypes, residual, coefficients):
    samples, phenotypes = residual.shape
    rows_own = coefficients.shape[0]
    whole = pl.BlockSpec(memory_space=pltpu.VMEM)
    far = pl.BlockSpec(memory_space=pltpu.HBM)
    return pl.pallas_call(
        head_kernel,
        out_shape=[
            jax.ShapeDtypeStruct((phenotypes, BS), F32),
            jax.ShapeDtypeStruct((2 * ROUNDS, BS), F32),
            jax.ShapeDtypeStruct((1, phenotypes), F32),
            jax.ShapeDtypeStruct((ROUNDS, rows_own, BS), F32),
        ],
        in_specs=[pl.BlockSpec(memory_space=pltpu.SMEM), far, far, far],
        out_specs=[whole] * 4,
        scratch_shapes=[
            pltpu.VMEM((ROUNDS, samples, BS), BF16),
            pltpu.VMEM((samples, phenotypes), F32),
            pltpu.SemaphoreType.DMA((ROUNDS, TILES)),
            pltpu.SemaphoreType.DMA,
            pltpu.SemaphoreType.DMA((ROUNDS,)),
        ],
        cost_estimate=pl.CostEstimate(
            flops=4 * samples * phenotypes * BS, bytes_accessed=4 * samples * BS, transcendentals=0
        ),
        compiler_params=pltpu.CompilerParams(vmem_limit_bytes=50 * 1024 * 1024),
        name="head",
    )(colors, genotypes, residual, coefficients)


def over_var(value):
    size = lax.axis_size("var")
    if size & (size - 1):
        total = lax.psum(value, "var")
        return total, jnp.zeros_like(total)
    step, other = 1, jnp.zeros_like(value)
    while step < size:
        value = value + other
        other = lax.ppermute(value.astype(BF16), "var", [(i, i ^ step) for i in range(size)]).astype(F32)
        value = rounded_to_bf16(value)
        step *= 2
    return value, other


def chosen_block(genotypes, block, gate):
    genotypes = after(genotypes, gate)
    return lax.optimization_barrier(lax.dynamic_slice_in_dim(genotypes, block * BS, BS, 1))


def descent(genotypes, residual, coefficients, penalty, colors):
    samp = lax.axis_size("samp")
    rows_own = coefficients.shape[0]
    phenotypes = rows_own * samp
    local_samples, total_samples = genotypes.shape[0], genotypes.shape[0] * samp
    width = BS // samp
    all_stages = stages(samp)
    early, last = all_stages[:-1], all_stages[-1]
    top = len(early) - 1
    chunks = 2 if phenotypes % 256 == 0 else 1
    size = phenotypes // chunks
    chosen = colors[:, 0]

    partial, stats, resid_sum, olds = head(colors, genotypes, residual, coefficients)
    partial_chunks = [partial[c * size : (c + 1) * size] for c in range(chunks)]
    sum_chunks = [resid_sum[0, c * size : (c + 1) * size] for c in range(chunks)]
    values = []

    first = jnp.int32(0)
    for stage in all_stages:
        first = first * stage.radix + stage.digit
    first = first * width

    def weights(r, gate):
        part = lax.dynamic_slice_in_dim(after(penalty, gate), chosen[r] * BS + first, width, 0)
        return lax.optimization_barrier(part)

    riders = [None] * (chunks - 1) + [jnp.concatenate(split_bf16(olds[0], 2), axis=0)]
    states = list(zip(partial_chunks, sum_chunks, riders))
    moments, samples = stats, local_samples
    sent_top, end_top, ends, members, gate = [], [], [], [None] * len(all_stages), ()
    for c in range(chunks):
        samples = local_samples
        for i in range(top + 1):
            sent, finish = merge_stage(early[i], *states[c], None if c else moments, samples)
            if i < top:
                states[c], members[i] = finish(gate, members[i])
                moments, samples = sum(members[i]), samples * early[i].radix
        sent_top.append(sent)
        end_top.append(finish)
        gate = sent
    gate = sent_top[-1]
    for c in range(chunks):
        states[c], members[top] = end_top[c](gate, members[top])
        if not c:
            moments, samples = sum(members[top]), samples * early[top].radix
        sent, finish = merge_stage(last, *states[c], None if c else moments, samples)
        ends.append(finish)
        gate = sent
    partial_chunks, members = [], None
    for finish in ends:
        (partial, _, riders), members = finish(gate, members)
        partial_chunks.append(partial)
    gradient = jnp.concatenate(partial_chunks, axis=0)
    moments = sum(members)
    old = jnp.sum(riders.astype(F32).reshape(samp, 2, rows_own, width), axis=1).reshape(phenotypes, width)
    ahead = sent_top[-1]
    weight = weights(0, ahead[0])
    values = [None] + [chosen_block(genotypes, chosen[r], ahead[0]) for r in range(1, ROUNDS)]
    old_later = jnp.stack([after(olds[r], *ahead) for r in range(1, ROUNDS)])
    for i in range(top):
        parts = send_parts(early[i], split_cols(old_later, early[i].radix))
        old_later = jnp.concatenate(in_order(early[i], *parts, sent), axis=-2)

    residuals = [residual[:, c * size : (c + 1) * size] for c in range(chunks)]
    news = []
    for r in range(ROUNDS):
        counts, twos = moments[2 * r], moments[2 * r + 1]
        mean = counts / total_samples
        scale = (counts + 2.0 * twos) - counts * mean
        if r:
            sent_top, end_top, ends = [], [], []
            for c in range(chunks):
                own, other = pending[c]
                if c:
                    other = after(other, *sent_top[-1])
                residuals[c] = residuals[c] - (own + other)
                rounded = residuals[c].astype(BF16)
                resid_sum = jnp.sum(rounded.astype(F32), axis=0)
                partial = lax.dot_general(rounded, values[r], (((0,), (0,)), ((), ())), preferred_element_type=F32)
                partial = partial - resid_sum[:, None] * means[r][None, :]
                for i in range(top + 1):
                    sent, finish = sum_stage(early[i], partial)
                    if i < top:
                        partial = finish()
                sent_top.append(sent)
                end_top.append(finish)
            gate = ahead = sent_top[-1]
            weight = weights(r, ahead[0])
            for c in range(chunks):
                partial = end_top[c](gate)
                gate, finish = sum_stage(last, partial)
                ends.append(finish)
            partial_chunks = [finish(gate) for finish in ends]
            old = jnp.concatenate(in_order(last, *old_parts, ahead), axis=-2)[r - 1]
            gradient = jnp.concatenate(partial_chunks, axis=0)
            for before in range(r):
                old = jnp.where(chosen[before] == chosen[r], news[before], old)
        shifted = old + gradient / scale[None, :]
        norm = jnp.sqrt(jnp.sum(shifted * shifted, axis=0) + 1e-06)
        shrink = jnp.maximum(0.0, 1.0 - weight * jnp.sqrt(phenotypes / scale) / norm)
        new = shrink[None, :] * shifted
        news.append(new)
        change = (new - old).astype(BF16)
        means_sent = [mean] if r else [moments[2 * i] / total_samples for i in range(ROUNDS)]
        rows = [row[None, :] for sent in means_sent for row in split_bf16(sent, 3)]
        rows = pad_rows(jnp.concatenate(rows, axis=0))
        lead = rows.shape[0]
        message = jnp.concatenate([rows, change], axis=0)
        if r == 0:
            values[0] = chosen_block(genotypes, chosen[0], message)
            old_parts = send_parts(early[top], split_cols(old_later, early[top].radix))
        gathered = gather_stage(message, last)
        cuts = [0] + [lead + size * (c + 1) for c in range(chunks)]
        pieces = [gathered[cuts[c] : cuts[c + 1]] for c in range(chunks)]
        received = []
        for c in range(chunks):
            received.append([early[top].send(pieces[c], step) for step in range(1, early[top].radix)])
        pending = []
        for c in range(chunks):
            if c:
                received[c] = [after(value, product) for value in received[c]]
            piece = jnp.concatenate(ordered(early[top], pieces[c], received[c]), axis=-1)
            for i in reversed(range(top)):
                piece = gather_stage(piece, early[i])
            if c == 0:
                rows, piece = piece[:lead], piece[lead:]
                if r == 0:
                    means = [jnp.sum(rows[3 * i : 3 * i + 3].astype(F32), axis=0) for i in range(ROUNDS)]
            shift = lax.dot_general(
                rows[:3], piece, (((1,), (1,)), ((), ())), preferred_element_type=F32
            )
            shift = jnp.sum(shift, axis=0)
            product = lax.dot_general(
                values[r], piece, (((1,), (1,)), ((), ())), preferred_element_type=F32
            )
            product = product - shift[None, :]
            pending.append(over_var(product))
        if r == 0:
            old_later = jnp.concatenate(in_order(early[top], *old_parts, [product]), axis=-2)
            old_parts = send_parts(last, split_cols(old_later, last.radix))

    for c in range(chunks):
        own, other = pending[c]
        residuals[c] = residuals[c] - (own + other)

    home = [new.reshape([stage.radix for stage in reversed(all_stages)] + [rows_own, width]) for new in news]
    home = jnp.stack(home, axis=len(all_stages))
    steps = [(top, 1, []), (top + 1, 1, [])] + [
        (i, len(all_stages) - 1 - i, []) for i in reversed(range(top))
    ]
    for i, axis, gate in steps:
        stage = all_stages[i]
        parts = [lax.index_in_dim(home, d, axis, keepdims=False) for d in range(stage.radix)]
        home = jnp.stack(in_order(stage, *send_parts(stage, parts), gate))
    found = list(range(top)) + [top + 1, top]
    home = jnp.transpose(home, [found.index(i) for i in range(len(found))] + [len(found) + j for j in range(3)])
    home = home.reshape(samp, ROUNDS, rows_own, width)
    new_rows = [jnp.concatenate([home[s, r] for s in range(samp)], axis=-1) for r in range(ROUNDS)]
    out = []
    for block in range(genotypes.shape[1] // BS):
        piece = coefficients[:, block * BS : (block + 1) * BS]
        for r in range(ROUNDS):
            piece = jnp.where(chosen[r] == block, new_rows[r], piece)
        out.append(piece)
    return (jnp.concatenate(out, axis=1), jnp.concatenate(residuals, axis=1))


def solution(mesh):
    placed = (P("samp", "var"), P("samp", None), P("samp", "var"), P("var"), P(None, "var"))
    return jax.shard_map(
        descent,
        mesh=mesh,
        in_specs=placed,
        out_specs=(P("samp", "var"), P("samp", None)),
        check_vma=False,
    )
```

```python
import functools

import jax
import jax.numpy as jnp
from jax import lax
from jax.experimental import pallas as pl
from jax.experimental.pallas import tpu as pltpu
from jax.sharding import PartitionSpec as P

BS = 2048
ROUNDS = 2
F32 = jnp.float32
BF16 = jnp.bfloat16


def stage_radices(size):
    radices = []
    while len(radices) < 2 and size % 2 == 0:
        radices.append(2)
        size //= 2
    if size > 1:
        radices.append(size)
    return radices


class Stage:
    def __init__(self, size, radix, stride):
        self.size, self.radix, self.stride = size, radix, stride
        digit = (lax.axis_index("samp") // stride) % radix
        self.mine = [digit == d for d in range(radix)]

    def partner(self, digit, step):
        if self.radix & (self.radix - 1) == 0:
            return digit ^ step
        return (digit + step) % self.radix

    def source(self, digit, step):
        if self.radix & (self.radix - 1) == 0:
            return digit ^ step
        return (digit - step) % self.radix

    def pairs(self, step):
        out = []
        for i in range(self.size):
            d = (i // self.stride) % self.radix
            out.append((i, i + (self.partner(d, step) - d) * self.stride))
        return out

    def send(self, value, step):
        return lax.ppermute(value, "samp", self.pairs(step))

    def by_digit(self, values):
        value = values[0]
        for d in range(1, self.radix):
            if values[d] is not value:
                value = jnp.where(self.mine[d], values[d], value)
        return value


def stages(size):
    out, stride = [], 1
    for radix in stage_radices(size):
        out.append(Stage(size, radix, stride))
        stride *= radix
    return out


def pick(parts, stage, step):
    return stage.by_digit([parts[stage.partner(d, step)] for d in range(stage.radix)])


def split_cols(value, radix):
    width = value.shape[-1] // radix
    return [value[..., i * width : (i + 1) * width] for i in range(radix)]


def ordered(stage, own, received):
    by_step = [own] + received
    step_of = [{stage.source(d, step): step for step in range(stage.radix)} for d in range(stage.radix)]
    return [stage.by_digit([by_step[step_of[d][o]] for d in range(stage.radix)]) for o in range(stage.radix)]


def rounded_to_bf16(value):
    return lax.reduce_precision(value, 8, 7)


def split_bf16(value, terms):
    out = []
    for _ in range(terms):
        top = rounded_to_bf16(value)
        out.append(top)
        value = value - top
    return out


def after(value, *others):
    return lax.optimization_barrier((value, *others))[0]


def send_parts(stage, parts):
    own = pick(parts, stage, 0)
    sent = [pick(parts, stage, step) for step in range(1, stage.radix)]
    return own, [stage.send(sent[step - 1], step) for step in range(1, stage.radix)]


def in_order(stage, own, received, gate=()):
    return ordered(stage, own, [after(value, *gate) for value in received])


def gather_stage(value, stage, gate=()):
    received = [after(stage.send(value, step), *gate) for step in range(1, stage.radix)]
    return jnp.concatenate(ordered(stage, value, received), axis=-1)


def stack_rows(rows):
    height = -(-len(rows) // 16) * 16
    at = lax.broadcasted_iota(jnp.int32, (height, rows[0].shape[0]), 0)
    out = jnp.zeros(at.shape, F32)
    for i, row in enumerate(rows):
        out = jnp.where(at == i, row[None, :], out)
    return out.astype(BF16)


def sum_rows(resid_sum, width):
    fit = min(width, resid_sum.shape[0])
    rows = [term.reshape(-1, fit)[i] for term in split_bf16(resid_sum, 3) for i in range(resid_sum.shape[0] // fit)]
    return [jnp.pad(row, (0, width - fit)) for row in rows]


def read_sums(rows, width, size):
    fit = min(width, size)
    return jnp.sum(rows.astype(F32).reshape(3, size // fit, width)[:, :, :fit], axis=0).reshape(size)


def merge_stage(stage, partial, resid_sum, riders, stats, samples):
    size, width = partial.shape[0], partial.shape[1] // stage.radix
    parts = split_cols(partial, stage.radix)
    sums = sum_rows(resid_sum, width)
    n_sum = len(sums)
    stat_parts = None if stats is None else split_cols(stats, stage.radix)
    rider_parts = None if riders is None else split_cols(riders, stage.radix)
    sent, arrived = [], []
    for step in range(1, stage.radix):
        extra = sums
        if stats is not None:
            terms = split_bf16(pick(stat_parts, stage, step), 2)
            extra = sums + [term[i] for term in terms for i in range(stats.shape[0])]
        message = [pick(parts, stage, step).astype(BF16), stack_rows(extra)]
        n_extra = message[1].shape[0]
        if riders is not None:
            message.append(pick(rider_parts, stage, step))
        sent.append(jnp.concatenate(message, axis=0))
        arrived.append(stage.send(sent[-1], step))

    def finish(gate=(), members=None):
        partials, resid_sums, ridden = [pick(parts, stage, 0)], [resid_sum], []
        if stats is not None:
            n_stats = stats.shape[0]
            members = [pick(stat_parts, stage, 0)]
        for message in arrived:
            message = after(message, *gate)
            partials.append(message[:size].astype(F32))
            tail = message[size:]
            ridden.append(tail[n_extra:])
            resid_sums.append(read_sums(tail[:n_sum], width, size))
            if stats is not None:
                terms = tail[n_sum : n_sum + 2 * n_stats].astype(F32)
                members.append(terms[:n_stats] + terms[n_stats:])
        count_mean = sum(m[0] for m in members) / stage.radix
        sum_mean = sum(resid_sums) / stage.radix
        total = sum(partials)
        for s, m in zip(resid_sums, members):
            total = total + (s - sum_mean)[:, None] * ((m[0] - count_mean) / samples)[None, :]
        merged = None
        if riders is not None:
            merged = jnp.concatenate(ordered(stage, pick(rider_parts, stage, 0), ridden), axis=0)
        return (total, sum(resid_sums), merged), members

    return sent, finish


def sum_stage(stage, partial):
    parts = split_cols(partial, stage.radix)
    own = pick(parts, stage, 0)
    sent = [pick(parts, stage, step).astype(BF16) for step in range(1, stage.radix)]
    arrived = [stage.send(sent[step - 1], step) for step in range(1, stage.radix)]

    def finish(gate=()):
        return sum((after(value, *gate).astype(F32) for value in arrived), start=own)

    return sent, finish


TILES = 4
BLOCK_LIMIT = 46
GROUP = 64


def column_moments(values):
    rows, width = values.shape
    whole = rows // 16 * 16
    counts = jnp.zeros((1, width), F32)
    twos = jnp.zeros((1, width), F32)
    one, zero = jnp.bfloat16(1), jnp.bfloat16(0)
    for begin in range(0, whole, 16 * GROUP):
        count_sum = two_sum = None
        for at in range(begin, min(begin + 16 * GROUP, whole), 16):
            part = values[at : at + 16]
            above = jnp.maximum(part - one, zero)
            count_sum = part if count_sum is None else count_sum + part
            two_sum = above if two_sum is None else two_sum + above
        counts = counts + jnp.sum(count_sum.astype(F32), axis=0, keepdims=True)
        twos = twos + jnp.sum(two_sum.astype(F32), axis=0, keepdims=True)
    if whole < rows:
        part = values[whole:].astype(F32)
        counts = counts + jnp.sum(part, axis=0, keepdims=True)
        twos = twos + jnp.sum(jnp.maximum(part - 1.0, 0.0), axis=0, keepdims=True)
    return counts, twos


def head_kernel(colors, genotypes, residual, partial, stats, resid_sum, chosen, blocks, sems):
    samples, phenotypes = residual.shape
    width = BS // TILES

    def copy(r, t):
        at = pl.multiple_of(colors[r] * BS + t * width, width)
        return pltpu.make_async_copy(
            genotypes.at[:, pl.ds(at, width)], blocks.at[r, :, pl.ds(t * width, width)], sems.at[r, t]
        )

    for r in range(ROUNDS):
        for t in range(TILES):
            copy(r, t).start()
    chosen[...] = jnp.zeros_like(chosen)
    for r in range(ROUNDS):
        chosen[r : r + 1, :] = jnp.full((1, chosen.shape[1]), colors[r], jnp.int32)
    rounded = residual[...].astype(BF16)
    sums = jnp.sum(rounded.astype(F32), axis=0, keepdims=True)
    resid_sum[...] = sums
    column = jnp.broadcast_to(jnp.transpose(jnp.broadcast_to(sums, (8, phenotypes)))[:, :1], (phenotypes, width))
    for r in range(ROUNDS):
        for t in range(TILES):
            copy(r, t).wait()
            here = pl.ds(t * width, width)
            values = blocks[r, :, here]
            counts, twos = column_moments(values)
            stats[2 * r : 2 * r + 1, here] = counts
            stats[2 * r + 1 : 2 * r + 2, here] = twos
            if r == 0:
                product = lax.dot_general(
                    rounded, values, (((0,), (0,)), ((), ())), preferred_element_type=F32
                )
                partial[:, here] = product - column * (counts * (1.0 / samples))


def head(colors, genotypes, residual):
    samples, phenotypes = residual.shape
    whole = pl.BlockSpec(memory_space=pltpu.VMEM)
    return pl.pallas_call(
        head_kernel,
        out_shape=[
            jax.ShapeDtypeStruct((phenotypes, BS), F32),
            jax.ShapeDtypeStruct((2 * ROUNDS, BS), F32),
            jax.ShapeDtypeStruct((1, phenotypes), F32),
            jax.ShapeDtypeStruct((8, 128), jnp.int32),
        ],
        in_specs=[pl.BlockSpec(memory_space=pltpu.SMEM), pl.BlockSpec(memory_space=pltpu.HBM), whole],
        out_specs=[whole] * 4,
        scratch_shapes=[
            pltpu.VMEM((ROUNDS, samples, BS), BF16),
            pltpu.SemaphoreType.DMA((ROUNDS, TILES)),
        ],
        cost_estimate=pl.CostEstimate(
            flops=4 * samples * phenotypes * BS, bytes_accessed=4 * samples * BS, transcendentals=0
        ),
        compiler_params=pltpu.CompilerParams(vmem_limit_bytes=50 * 1024 * 1024),
        name="head",
    )(colors, genotypes, residual)


def over_var(value):
    size = lax.axis_size("var")
    if size & (size - 1):
        total = lax.psum(value, "var")
        return total, jnp.zeros_like(total)
    step, other = 1, jnp.zeros_like(value)
    while step < size:
        value = value + other
        other = lax.ppermute(value.astype(BF16), "var", [(i, i ^ step) for i in range(size)]).astype(F32)
        value = rounded_to_bf16(value)
        step *= 2
    return value, other


def block_kernel(r, colors, genotypes, block, sems):
    width = BS // TILES
    copies = []
    for t in range(TILES):
        at = pl.multiple_of(colors[r] * BS + t * width, width)
        copies.append(
            pltpu.make_async_copy(
                genotypes.at[:, pl.ds(at, width)], block.at[:, pl.ds(t * width, width)], sems.at[t]
            )
        )
    for copy in copies:
        copy.start()
    for copy in copies:
        copy.wait()


def chosen_block(colors, genotypes, r, gate):
    samples = genotypes.shape[0]
    return pl.pallas_call(
        functools.partial(block_kernel, r),
        out_shape=jax.ShapeDtypeStruct((samples, BS), BF16),
        in_specs=[pl.BlockSpec(memory_space=pltpu.SMEM), pl.BlockSpec(memory_space=pltpu.HBM)],
        out_specs=pl.BlockSpec(memory_space=pltpu.VMEM),
        scratch_shapes=[pltpu.SemaphoreType.DMA((TILES,))],
        cost_estimate=pl.CostEstimate(flops=10**9, bytes_accessed=2 * samples * BS, transcendentals=0),
        compiler_params=pltpu.CompilerParams(vmem_limit_bytes=BLOCK_LIMIT * 1024 * 1024),
    )(after(colors, gate), genotypes)


def descent(genotypes, residual, coefficients, penalty, colors):
    samp = lax.axis_size("samp")
    rows_own = coefficients.shape[0]
    phenotypes = rows_own * samp
    local_samples, total_samples = genotypes.shape[0], genotypes.shape[0] * samp
    width = BS // samp
    all_stages = stages(samp)
    early, last = all_stages[:-1], all_stages[-1]
    top = len(early) - 1
    chunks = 2 if phenotypes % 256 == 0 else 1
    size = phenotypes // chunks
    n_blocks = genotypes.shape[1] // BS
    colors = colors[:, 0]

    first = jnp.int32(0)
    for stage in all_stages:
        digit = sum(d * mine.astype(jnp.int32) for d, mine in enumerate(stage.mine))
        first = first * stage.radix + digit
    first = [(first * width + block * BS).astype(jnp.uint32) for block in range(n_blocks)]
    mine = [stage.mine for stage in all_stages]
    genotypes, first, mine = lax.optimization_barrier((genotypes, first, mine))
    for stage, flags in zip(all_stages, mine):
        stage.mine = flags

    partial, stats, resid_sum, chosen = head(colors, genotypes, residual)
    partial_chunks = [partial[c * size : (c + 1) * size] for c in range(chunks)]
    sum_chunks = [resid_sum[0, c * size : (c + 1) * size] for c in range(chunks)]
    chosen = [chosen[r : r + 1, :1] for r in range(ROUNDS)]

    def of_block(array, r):
        parts = split_cols(array, n_blocks)
        value = parts[0]
        for block in range(1, n_blocks):
            value = jnp.where(chosen[r] == block, parts[block], value)
        return value

    olds = [of_block(coefficients, r) for r in range(ROUNDS)]

    def weights(r, gate):
        held = after(penalty, gate)
        parts = [lax.dynamic_slice(held, (at,), (width,)) for at in first]
        parts = lax.optimization_barrier(parts)
        value = parts[0][None, :]
        for block in range(1, n_blocks):
            value = jnp.where(chosen[r] == block, parts[block][None, :], value)
        return value[0]

    riders = [None] * (chunks - 1) + [jnp.concatenate(split_bf16(olds[0], 2), axis=0).astype(BF16)]
    states = list(zip(partial_chunks, sum_chunks, riders))
    moments, samples = stats, local_samples
    sent_top, end_top, ends, members, gate = [], [], [], [None] * len(all_stages), ()
    for c in range(chunks):
        samples = local_samples
        for i in range(top + 1):
            sent, finish = merge_stage(early[i], *states[c], None if c else moments, samples)
            if i < top:
                states[c], members[i] = finish(gate, members[i])
                moments, samples = sum(members[i]), samples * early[i].radix
        sent_top.append(sent)
        end_top.append(finish)
        gate = sent
    gate = sent_top[-1]
    for c in range(chunks):
        states[c], members[top] = end_top[c](gate, members[top])
        if not c:
            moments, samples = sum(members[top]), samples * early[top].radix
        sent, finish = merge_stage(last, *states[c], None if c else moments, samples)
        ends.append(finish)
        gate = sent
    partial_chunks, members = [], None
    for finish in ends:
        (partial, _, riders), members = finish(gate, members)
        partial_chunks.append(partial)
    gradient = jnp.concatenate(partial_chunks, axis=0)
    moments = sum(members)
    old = jnp.sum(riders.astype(F32).reshape(samp, 2, rows_own, width), axis=1).reshape(phenotypes, width)
    ahead = sent_top[-1]
    weight = weights(0, ahead[0])
    values = [None] + [chosen_block(colors, genotypes, r, ahead[0]) for r in range(1, ROUNDS)]
    old_later = jnp.stack([after(olds[r], *ahead) for r in range(1, ROUNDS)])
    for i in range(top):
        parts = send_parts(early[i], split_cols(old_later, early[i].radix))
        old_later = jnp.concatenate(in_order(early[i], *parts, sent), axis=-2)

    residuals = [residual[:, c * size : (c + 1) * size] for c in range(chunks)]
    news = []
    for r in range(ROUNDS):
        counts, twos = moments[2 * r], moments[2 * r + 1]
        mean = counts / total_samples
        scale = (counts + 2.0 * twos) - counts * mean
        if r:
            sent_top, end_top, ends = [], [], []
            for c in range(chunks):
                own, other = pending[c]
                if c:
                    other = after(other, *sent_top[-1])
                residuals[c] = residuals[c] - (own + other)
                rounded = residuals[c].astype(BF16)
                resid_sum = jnp.sum(rounded.astype(F32), axis=0)
                partial = lax.dot_general(rounded, values[r], (((0,), (0,)), ((), ())), preferred_element_type=F32)
                partial = partial - resid_sum[:, None] * means[r][None, :]
                for i in range(top + 1):
                    sent, finish = sum_stage(early[i], partial)
                    if i < top:
                        partial = finish()
                sent_top.append(sent)
                end_top.append(finish)
            gate = ahead = sent_top[-1]
            weight = weights(r, ahead[0])
            for c in range(chunks):
                partial = end_top[c](gate)
                gate, finish = sum_stage(last, partial)
                ends.append(finish)
            partial_chunks = [finish(gate) for finish in ends]
            old = jnp.concatenate(in_order(last, *old_parts, ahead), axis=-2)[r - 1]
            gradient = jnp.concatenate(partial_chunks, axis=0)
            for before in range(r):
                old = jnp.where(chosen[before] == chosen[r], news[before], old)
        shifted = old + gradient / scale[None, :]
        norm = jnp.sqrt(jnp.sum(shifted * shifted, axis=0) + 1e-06)
        shrink = jnp.maximum(0.0, 1.0 - weight * jnp.sqrt(phenotypes / scale) / norm)
        new = shrink[None, :] * shifted
        news.append(new)
        change = (new - old).astype(BF16)
        means_sent = [mean] if r else [moments[2 * i] / total_samples for i in range(ROUNDS)]
        rows = stack_rows([row for sent in means_sent for row in split_bf16(sent, 3)])
        lead = rows.shape[0]
        message = jnp.concatenate([rows, change], axis=0)
        if r == 0:
            values[0] = chosen_block(colors, genotypes, 0, message)
            old_parts = send_parts(early[top], split_cols(old_later, early[top].radix))
        gathered = gather_stage(message, last)
        cuts = [0] + [lead + size * (c + 1) for c in range(chunks)]
        pieces = [gathered[cuts[c] : cuts[c + 1]] for c in range(chunks)]
        received = []
        for c in range(chunks):
            received.append([early[top].send(pieces[c], step) for step in range(1, early[top].radix)])
        pending = []
        for c in range(chunks):
            if c:
                received[c] = [after(value, product) for value in received[c]]
            piece = jnp.concatenate(ordered(early[top], pieces[c], received[c]), axis=-1)
            for i in reversed(range(top)):
                piece = gather_stage(piece, early[i])
            if c == 0:
                rows, piece = piece[:lead], piece[lead:]
                if r == 0:
                    means = [jnp.sum(rows[3 * i : 3 * i + 3].astype(F32), axis=0) for i in range(ROUNDS)]
            shift = lax.dot_general(
                rows[:3], piece, (((1,), (1,)), ((), ())), preferred_element_type=F32
            )
            shift = jnp.sum(shift, axis=0)
            product = lax.dot_general(
                values[r], piece, (((1,), (1,)), ((), ())), preferred_element_type=F32
            )
            product = product - shift[None, :]
            pending.append(over_var(product))
        if r == 0:
            old_later = jnp.concatenate(in_order(early[top], *old_parts, [product]), axis=-2)
            old_parts = send_parts(last, split_cols(old_later, last.radix))

    for c in range(chunks):
        own, other = pending[c]
        residuals[c] = residuals[c] - (own + other)

    home = [new.reshape([stage.radix for stage in reversed(all_stages)] + [rows_own, width]) for new in news]
    home = jnp.stack(home, axis=len(all_stages))
    steps = [(top, 1, []), (top + 1, 1, [])] + [
        (i, len(all_stages) - 1 - i, []) for i in reversed(range(top))
    ]
    for i, axis, gate in steps:
        stage = all_stages[i]
        parts = [lax.index_in_dim(home, d, axis, keepdims=False) for d in range(stage.radix)]
        home = jnp.stack(in_order(stage, *send_parts(stage, parts), gate))
    found = list(range(top)) + [top + 1, top]
    home = jnp.transpose(home, [found.index(i) for i in range(len(found))] + [len(found) + j for j in range(3)])
    home = home.reshape(samp, ROUNDS, rows_own, width)
    new_rows = [jnp.concatenate([home[s, r] for s in range(samp)], axis=-1) for r in range(ROUNDS)]
    out = []
    for block in range(n_blocks):
        piece = coefficients[:, block * BS : (block + 1) * BS]
        for r in range(ROUNDS):
            piece = jnp.where(chosen[r] == block, new_rows[r], piece)
        out.append(piece)
    return (jnp.concatenate(out, axis=1), jnp.concatenate(residuals, axis=1))


def solution(mesh):
    placed = (P("samp", "var"), P("samp", None), P("samp", "var"), P("var"), P(None, "var"))
    return jax.shard_map(
        descent,
        mesh=mesh,
        in_specs=placed,
        out_specs=(P("samp", "var"), P("samp", None)),
        check_vma=False,
    )
```

```python
import functools

import jax
import jax.numpy as jnp
from jax import lax
from jax.experimental import pallas as pl
from jax.experimental.pallas import tpu as pltpu
from jax.sharding import PartitionSpec as P

BS = 2048
ROUNDS = 2
F32 = jnp.float32
BF16 = jnp.bfloat16


def stage_radices(size):
    radices = []
    while len(radices) < 2 and size % 2 == 0:
        radices.append(2)
        size //= 2
    if size > 1:
        radices.append(size)
    return radices


class Stage:
    def __init__(self, size, radix, stride):
        self.size, self.radix, self.stride = size, radix, stride
        digit = (lax.axis_index("samp") // stride) % radix
        self.mine = [digit == d for d in range(radix)]

    def partner(self, digit, step):
        if self.radix & (self.radix - 1) == 0:
            return digit ^ step
        return (digit + step) % self.radix

    def source(self, digit, step):
        if self.radix & (self.radix - 1) == 0:
            return digit ^ step
        return (digit - step) % self.radix

    def pairs(self, step):
        out = []
        for i in range(self.size):
            d = (i // self.stride) % self.radix
            out.append((i, i + (self.partner(d, step) - d) * self.stride))
        return out

    def send(self, value, step):
        return lax.ppermute(value, "samp", self.pairs(step))

    def by_digit(self, values):
        value = values[0]
        for d in range(1, self.radix):
            if values[d] is not value:
                value = jnp.where(self.mine[d], values[d], value)
        return value


def stages(size):
    out, stride = [], 1
    for radix in stage_radices(size):
        out.append(Stage(size, radix, stride))
        stride *= radix
    return out


def pick(parts, stage, step):
    return stage.by_digit([parts[stage.partner(d, step)] for d in range(stage.radix)])


def split_cols(value, radix):
    width = value.shape[-1] // radix
    return [value[..., i * width : (i + 1) * width] for i in range(radix)]


def ordered(stage, own, received):
    by_step = [own] + received
    step_of = [{stage.source(d, step): step for step in range(stage.radix)} for d in range(stage.radix)]
    return [stage.by_digit([by_step[step_of[d][o]] for d in range(stage.radix)]) for o in range(stage.radix)]


def rounded_to_bf16(value):
    return lax.reduce_precision(value, 8, 7)


def split_bf16(value, terms):
    out = []
    for _ in range(terms):
        top = rounded_to_bf16(value)
        out.append(top)
        value = value - top
    return out


def after(value, *others):
    return lax.optimization_barrier((value, *others))[0]


def send_parts(stage, parts):
    own = pick(parts, stage, 0)
    sent = [pick(parts, stage, step) for step in range(1, stage.radix)]
    return own, [stage.send(sent[step - 1], step) for step in range(1, stage.radix)]


def in_order(stage, own, received, gate=()):
    return ordered(stage, own, [after(value, *gate) for value in received])


def gather_stage(value, stage, gate=()):
    received = [after(stage.send(value, step), *gate) for step in range(1, stage.radix)]
    return jnp.concatenate(ordered(stage, value, received), axis=-1)


def stack_rows(rows):
    height = -(-len(rows) // 16) * 16
    at = lax.broadcasted_iota(jnp.int32, (height, rows[0].shape[0]), 0)
    out = jnp.zeros(at.shape, F32)
    for i, row in enumerate(rows):
        out = jnp.where(at == i, row[None, :], out)
    return out.astype(BF16)


def sum_rows(resid_sum, width):
    fit = min(width, resid_sum.shape[0])
    rows = [term.reshape(-1, fit)[i] for term in split_bf16(resid_sum, 3) for i in range(resid_sum.shape[0] // fit)]
    return [jnp.pad(row, (0, width - fit)) for row in rows]


def read_sums(rows, width, size):
    fit = min(width, size)
    return jnp.sum(rows.astype(F32).reshape(3, size // fit, width)[:, :, :fit], axis=0).reshape(size)


def merge_stage(stage, partial, resid_sum, riders, stats, samples):
    size, width = partial.shape[0], partial.shape[1] // stage.radix
    parts = split_cols(partial, stage.radix)
    sums = sum_rows(resid_sum, width)
    n_sum = len(sums)
    stat_parts = None if stats is None else split_cols(stats, stage.radix)
    rider_parts = None if riders is None else split_cols(riders, stage.radix)
    sent, arrived = [], []
    for step in range(1, stage.radix):
        extra = sums
        if stats is not None:
            terms = split_bf16(pick(stat_parts, stage, step), 2)
            extra = sums + [term[i] for term in terms for i in range(stats.shape[0])]
        message = [pick(parts, stage, step).astype(BF16), stack_rows(extra)]
        n_extra = message[1].shape[0]
        if riders is not None:
            message.append(pick(rider_parts, stage, step))
        sent.append(jnp.concatenate(message, axis=0))
        arrived.append(stage.send(sent[-1], step))

    def finish(gate=(), members=None):
        partials, resid_sums, ridden = [pick(parts, stage, 0)], [resid_sum], []
        if stats is not None:
            n_stats = stats.shape[0]
            members = [pick(stat_parts, stage, 0)]
        for message in arrived:
            message = after(message, *gate)
            partials.append(message[:size].astype(F32))
            tail = message[size:]
            ridden.append(tail[n_extra:])
            resid_sums.append(read_sums(tail[:n_sum], width, size))
            if stats is not None:
                terms = tail[n_sum : n_sum + 2 * n_stats].astype(F32)
                members.append(terms[:n_stats] + terms[n_stats:])
        count_mean = sum(m[0] for m in members) / stage.radix
        sum_mean = sum(resid_sums) / stage.radix
        total = sum(partials)
        for s, m in zip(resid_sums, members):
            total = total + (s - sum_mean)[:, None] * ((m[0] - count_mean) / samples)[None, :]
        merged = None
        if riders is not None:
            merged = jnp.concatenate(ordered(stage, pick(rider_parts, stage, 0), ridden), axis=0)
        return (total, sum(resid_sums), merged), members

    return sent, finish


def sum_stage(stage, partial):
    parts = split_cols(partial, stage.radix)
    own = pick(parts, stage, 0)
    sent = [pick(parts, stage, step).astype(BF16) for step in range(1, stage.radix)]
    arrived = [stage.send(sent[step - 1], step) for step in range(1, stage.radix)]

    def finish(gate=()):
        return sum((after(value, *gate).astype(F32) for value in arrived), start=own)

    return sent, finish


TILES = 4
BLOCK_LIMIT = 46
GROUP = 64


def column_moments(values):
    rows, width = values.shape
    whole = rows // 16 * 16
    counts = jnp.zeros((1, width), F32)
    twos = jnp.zeros((1, width), F32)
    one, zero = jnp.bfloat16(1), jnp.bfloat16(0)
    for begin in range(0, whole, 16 * GROUP):
        count_sum = two_sum = None
        for at in range(begin, min(begin + 16 * GROUP, whole), 16):
            part = values[at : at + 16]
            above = jnp.maximum(part - one, zero)
            count_sum = part if count_sum is None else count_sum + part
            two_sum = above if two_sum is None else two_sum + above
        counts = counts + jnp.sum(count_sum.astype(F32), axis=0, keepdims=True)
        twos = twos + jnp.sum(two_sum.astype(F32), axis=0, keepdims=True)
    if whole < rows:
        part = values[whole:].astype(F32)
        counts = counts + jnp.sum(part, axis=0, keepdims=True)
        twos = twos + jnp.sum(jnp.maximum(part - 1.0, 0.0), axis=0, keepdims=True)
    return counts, twos


def head_kernel(colors, genotypes, residual, partial, stats, resid_sum, chosen, blocks, sems):
    samples, phenotypes = residual.shape
    width = BS // TILES

    def copy(r, t):
        at = pl.multiple_of(colors[r] * BS + t * width, width)
        return pltpu.make_async_copy(
            genotypes.at[:, pl.ds(at, width)], blocks.at[r, :, pl.ds(t * width, width)], sems.at[r, t]
        )

    for r in range(ROUNDS):
        for t in range(TILES):
            copy(r, t).start()
    chosen[...] = jnp.zeros_like(chosen)
    for r in range(ROUNDS):
        chosen[r : r + 1, :] = jnp.full((1, chosen.shape[1]), colors[r], jnp.int32)
    rounded = residual[...].astype(BF16)
    sums = jnp.sum(rounded.astype(F32), axis=0, keepdims=True)
    resid_sum[...] = sums
    column = jnp.broadcast_to(jnp.transpose(jnp.broadcast_to(sums, (8, phenotypes)))[:, :1], (phenotypes, width))
    for r in range(ROUNDS):
        for t in range(TILES):
            copy(r, t).wait()
            here = pl.ds(t * width, width)
            values = blocks[r, :, here]
            counts, twos = column_moments(values)
            stats[2 * r : 2 * r + 1, here] = counts
            stats[2 * r + 1 : 2 * r + 2, here] = twos
            if r == 0:
                product = lax.dot_general(
                    rounded, values, (((0,), (0,)), ((), ())), preferred_element_type=F32
                )
                partial[:, here] = product - column * (counts * (1.0 / samples))


def head(colors, genotypes, residual):
    samples, phenotypes = residual.shape
    whole = pl.BlockSpec(memory_space=pltpu.VMEM)
    return pl.pallas_call(
        head_kernel,
        out_shape=[
            jax.ShapeDtypeStruct((phenotypes, BS), F32),
            jax.ShapeDtypeStruct((2 * ROUNDS, BS), F32),
            jax.ShapeDtypeStruct((1, phenotypes), F32),
            jax.ShapeDtypeStruct((8, 128), jnp.int32),
        ],
        in_specs=[pl.BlockSpec(memory_space=pltpu.SMEM), pl.BlockSpec(memory_space=pltpu.HBM), whole],
        out_specs=[whole] * 4,
        scratch_shapes=[
            pltpu.VMEM((ROUNDS, samples, BS), BF16),
            pltpu.SemaphoreType.DMA((ROUNDS, TILES)),
        ],
        cost_estimate=pl.CostEstimate(
            flops=4 * samples * phenotypes * BS, bytes_accessed=4 * samples * BS, transcendentals=0
        ),
        compiler_params=pltpu.CompilerParams(vmem_limit_bytes=50 * 1024 * 1024),
        name="head",
    )(colors, genotypes, residual)


def over_var(value):
    size = lax.axis_size("var")
    if size & (size - 1):
        total = lax.psum(value, "var")
        return total, jnp.zeros_like(total)
    step, other = 1, jnp.zeros_like(value)
    while step < size:
        value = value + other
        other = lax.ppermute(value.astype(BF16), "var", [(i, i ^ step) for i in range(size)]).astype(F32)
        value = rounded_to_bf16(value)
        step *= 2
    return value, other


def block_kernel(r, colors, genotypes, block, sems):
    width = BS // TILES
    copies = []
    for t in range(TILES):
        at = pl.multiple_of(colors[r] * BS + t * width, width)
        copies.append(
            pltpu.make_async_copy(
                genotypes.at[:, pl.ds(at, width)], block.at[:, pl.ds(t * width, width)], sems.at[t]
            )
        )
    for copy in copies:
        copy.start()
    for copy in copies:
        copy.wait()


def chosen_block(colors, genotypes, r, gate):
    samples = genotypes.shape[0]
    return pl.pallas_call(
        functools.partial(block_kernel, r),
        out_shape=jax.ShapeDtypeStruct((samples, BS), BF16),
        in_specs=[pl.BlockSpec(memory_space=pltpu.SMEM), pl.BlockSpec(memory_space=pltpu.HBM)],
        out_specs=pl.BlockSpec(memory_space=pltpu.VMEM),
        scratch_shapes=[pltpu.SemaphoreType.DMA((TILES,))],
        cost_estimate=pl.CostEstimate(flops=10**9, bytes_accessed=2 * samples * BS, transcendentals=0),
        compiler_params=pltpu.CompilerParams(vmem_limit_bytes=BLOCK_LIMIT * 1024 * 1024),
    )(after(colors, gate), genotypes)


def descent(genotypes, residual, coefficients, penalty, colors):
    samp = lax.axis_size("samp")
    rows_own = coefficients.shape[0]
    phenotypes = rows_own * samp
    local_samples, total_samples = genotypes.shape[0], genotypes.shape[0] * samp
    width = BS // samp
    all_stages = stages(samp)
    early, last = all_stages[:-1], all_stages[-1]
    top = len(early) - 1
    chunks = 2 if phenotypes % 256 == 0 else 1
    size = phenotypes // chunks
    n_blocks = genotypes.shape[1] // BS
    colors = colors[:, 0]

    first = jnp.int32(0)
    for stage in all_stages:
        digit = sum(d * mine.astype(jnp.int32) for d, mine in enumerate(stage.mine))
        first = first * stage.radix + digit
    first = [(first * width + block * BS).astype(jnp.uint32) for block in range(n_blocks)]
    mine = [stage.mine for stage in all_stages]
    genotypes, first, mine = lax.optimization_barrier((genotypes, first, mine))
    for stage, flags in zip(all_stages, mine):
        stage.mine = flags

    partial, stats, resid_sum, chosen = head(colors, genotypes, residual)
    partial_chunks = [partial[c * size : (c + 1) * size] for c in range(chunks)]
    sum_chunks = [resid_sum[0, c * size : (c + 1) * size] for c in range(chunks)]
    chosen = [chosen[r : r + 1, :1] for r in range(ROUNDS)]

    def of_block(array, r):
        parts = split_cols(array, n_blocks)
        value = parts[0]
        for block in range(1, n_blocks):
            value = jnp.where(chosen[r] == block, parts[block], value)
        return value

    olds = [of_block(coefficients, r) for r in range(ROUNDS)]

    def weights(r, gate):
        held = after(penalty, gate)
        parts = [lax.dynamic_slice(held, (at,), (width,)) for at in first]
        parts = lax.optimization_barrier(parts)
        value = parts[0][None, :]
        for block in range(1, n_blocks):
            value = jnp.where(chosen[r] == block, parts[block][None, :], value)
        return value[0]

    riders = [None] * (chunks - 1) + [jnp.concatenate(split_bf16(olds[0], 2), axis=0).astype(BF16)]
    states = list(zip(partial_chunks, sum_chunks, riders))
    moments, samples = stats, local_samples
    sent_top, end_top, ends, members, gate = [], [], [], [None] * len(all_stages), ()
    for c in range(chunks):
        samples = local_samples
        for i in range(top + 1):
            sent, finish = merge_stage(early[i], *states[c], None if c else moments, samples)
            if i < top:
                states[c], members[i] = finish(gate, members[i])
                moments, samples = sum(members[i]), samples * early[i].radix
        sent_top.append(sent)
        end_top.append(finish)
        gate = sent
    gate = sent_top[-1]
    for c in range(chunks):
        states[c], members[top] = end_top[c](gate, members[top])
        if not c:
            moments, samples = sum(members[top]), samples * early[top].radix
        sent, finish = merge_stage(last, *states[c], None if c else moments, samples)
        ends.append(finish)
        gate = sent
    partial_chunks, members = [], None
    for finish in ends:
        (partial, _, riders), members = finish(gate, members)
        partial_chunks.append(partial)
    gradient = jnp.concatenate(partial_chunks, axis=0)
    moments = sum(members)
    old = jnp.sum(riders.astype(F32).reshape(samp, 2, rows_own, width), axis=1).reshape(phenotypes, width)
    ahead = sent_top[-1]
    weight = weights(0, ahead[0])
    values = [None] + [chosen_block(colors, genotypes, r, ahead[0]) for r in range(1, ROUNDS)]
    old_later = jnp.stack([after(olds[r], *ahead) for r in range(1, ROUNDS)])
    for i in range(top):
        parts = send_parts(early[i], split_cols(old_later, early[i].radix))
        old_later = jnp.concatenate(in_order(early[i], *parts, sent), axis=-2)

    residuals = [residual[:, c * size : (c + 1) * size] for c in range(chunks)]
    news = []
    for r in range(ROUNDS):
        counts, twos = moments[2 * r], moments[2 * r + 1]
        mean = counts / total_samples
        scale = (counts + 2.0 * twos) - counts * mean
        if r:
            sent_top, end_top, ends = [], [], []
            for c in range(chunks):
                own, other = pending[c]
                if c:
                    other = after(other, *sent_top[-1])
                residuals[c] = residuals[c] - (own + other)
                rounded = residuals[c].astype(BF16)
                resid_sum = jnp.sum(rounded.astype(F32), axis=0)
                partial = lax.dot_general(rounded, values[r], (((0,), (0,)), ((), ())), preferred_element_type=F32)
                partial = partial - resid_sum[:, None] * means[r][None, :]
                for i in range(top + 1):
                    sent, finish = sum_stage(early[i], partial)
                    if i < top:
                        partial = finish()
                sent_top.append(sent)
                end_top.append(finish)
            gate = ahead = sent_top[-1]
            weight = weights(r, ahead[0])
            for c in range(chunks):
                partial = end_top[c](gate)
                gate, finish = sum_stage(last, partial)
                ends.append(finish)
            partial_chunks = [finish(gate) for finish in ends]
            old = jnp.concatenate(in_order(last, *old_parts, ahead), axis=-2)[r - 1]
            gradient = jnp.concatenate(partial_chunks, axis=0)
            for before in range(r):
                old = jnp.where(chosen[before] == chosen[r], news[before], old)
        shifted = old + gradient / scale[None, :]
        norm = jnp.sqrt(jnp.sum(shifted * shifted, axis=0) + 1e-06)
        shrink = jnp.maximum(0.0, 1.0 - weight * jnp.sqrt(phenotypes / scale) / norm)
        new = shrink[None, :] * shifted
        news.append(new)
        change = (new - old).astype(BF16)
        means_sent = [mean] if r else [moments[2 * i] / total_samples for i in range(ROUNDS)]
        rows = stack_rows([row for sent in means_sent for row in split_bf16(sent, 3)])
        lead = rows.shape[0]
        message = jnp.concatenate([rows, change], axis=0)
        if r == 0:
            values[0] = chosen_block(colors, genotypes, 0, message)
            old_parts = send_parts(early[top], split_cols(old_later, early[top].radix))
        gathered = gather_stage(message, last)
        cuts = [0] + [lead + size * (c + 1) for c in range(chunks)]
        pieces = [gathered[cuts[c] : cuts[c + 1]] for c in range(chunks)]
        received = []
        for c in range(chunks):
            received.append([early[top].send(pieces[c], step) for step in range(1, early[top].radix)])
        pending = []
        for c in range(chunks):
            if c:
                received[c] = [after(value, product) for value in received[c]]
            piece = jnp.concatenate(ordered(early[top], pieces[c], received[c]), axis=-1)
            for i in reversed(range(top)):
                piece = gather_stage(piece, early[i])
            if c == 0:
                rows, piece = piece[:lead], piece[lead:]
                if r == 0:
                    means = [jnp.sum(rows[3 * i : 3 * i + 3].astype(F32), axis=0) for i in range(ROUNDS)]
            shift = lax.dot_general(
                rows[:3], piece, (((1,), (1,)), ((), ())), preferred_element_type=F32
            )
            shift = jnp.sum(shift, axis=0)
            product = lax.dot_general(
                values[r], piece, (((1,), (1,)), ((), ())), preferred_element_type=F32
            )
            product = product - shift[None, :]
            pending.append(over_var(product))
        if r == 0:
            old_later = jnp.concatenate(in_order(early[top], *old_parts, [product]), axis=-2)
            old_parts = send_parts(last, split_cols(old_later, last.radix))

    for c in range(chunks):
        own, other = pending[c]
        residuals[c] = residuals[c] - (own + other)

    home = [new.astype(BF16).reshape([stage.radix for stage in reversed(all_stages)] + [rows_own, width]) for new in news]
    home = jnp.stack(home, axis=len(all_stages))
    steps = [(top, 1, pieces[-1:]), (top + 1, 1, [])] + [
        (i, len(all_stages) - 1 - i, []) for i in reversed(range(top))
    ]
    for i, axis, gate in steps:
        stage = all_stages[i]
        parts = [lax.index_in_dim(home, d, axis, keepdims=False) for d in range(stage.radix)]
        home = jnp.stack(in_order(stage, *send_parts(stage, parts), gate))
    found = list(range(top)) + [top + 1, top]
    home = jnp.transpose(home, [found.index(i) for i in range(len(found))] + [len(found) + j for j in range(3)])
    home = home.reshape(samp, ROUNDS, rows_own, width)
    new_rows = [jnp.concatenate([home[s, r] for s in range(samp)], axis=-1).astype(F32) for r in range(ROUNDS)]
    out = []
    for block in range(n_blocks):
        piece = coefficients[:, block * BS : (block + 1) * BS]
        for r in range(ROUNDS):
            piece = jnp.where(chosen[r] == block, new_rows[r], piece)
        out.append(piece)
    return (jnp.concatenate(out, axis=1), jnp.concatenate(residuals, axis=1))


def solution(mesh):
    placed = (P("samp", "var"), P("samp", None), P("samp", "var"), P("var"), P(None, "var"))
    return jax.shard_map(
        descent,
        mesh=mesh,
        in_specs=placed,
        out_specs=(P("samp", "var"), P("samp", None)),
        check_vma=False,
    )
```
